256 devices in a mesh: space: 128 (over z, y, x), rep: 2 (over core).
Axes of the slice: x: 4, y: 4, z: 8, core: 2. Of those that a mesh axis runs over, the one named last changes fastest.
Arguments:
- halo_rows: bfloat16 [4, 16384, 256], P(None, 'space', 'rep'), may hold values from -6 to 6
- unmatched: int32 [4, 16384], P(None, 'space'), may hold values 0 or 1
- owner_id: int32 [4, 16384, 1], P(None, 'space'), may hold values from 0 to 127; in each aligned block of 128 rows (0 to 127, 128 to 255, ..., all dimensions but the last counted through in order) at most 2 rows name the same one
- cand_index: int32 [4, 16384, 16], P(None, 'space'), may hold values from 0 to 511
- lengths: int32 [4, 16384], P(None, 'space'), may hold values from 1 to 16
- choice_index: int32 [4, 16384], P(None, 'space'), may hold values from 0 to 15, as said below
- desc_rows: bfloat16 [4, 65536, 256], P(None, 'space', 'rep'), may hold values from -6 to 6
Outputs:
- phantom: bfloat16 [4, 16384, 256], P(None, 'space', 'rep')
- best_merit: bfloat16 [4, 16384], P(None, 'space')
The draws below stay inside these ranges and needn't reach their ends.
Inputs may be any that keep to these rules, and one draw needn't show every extreme that they name: `owner_id`: in each aligned block of 128 halos (one region in one snapshot) no owner is named by more than 2 halos, a bound that some block reaches. `choice_index`: less than the halo's length.
All inputs are finite; a program needn't handle non-finite values. No bound on the sum of `unmatched` on one device may be relied on, other than what follows from the above.
Results may differ from the reference program's by a relative error of at most 0.001.
Values may be sent and summed in bfloat16 or wider, within the bound.
A program may use at most 64 MiB of HBM per device.

```python
import math
import jax
import jax.numpy as jnp
import numpy as np
from jax import lax

WIDTH = 256
SNAPS = 4
K = 16
HALO_DEV = 128
CAND_DEV = 512
CAP = 2
HALOS = 16384
CANDS = 65536
N_SPACE = 128


def draw_pair(key):
    base_key = jax.random.fold_in(key, 71)
    first_key, second_key = jax.random.split(base_key)
    span_draw = jax.random.randint(first_key, (SNAPS, HALOS), 1, K + 1)
    pick_draw = jax.random.randint(second_key, (SNAPS, HALOS), 0, 1048576) % span_draw
    return (span_draw, pick_draw)


def draw_lengths(key, part):
    return draw_pair(key)[0].astype(jnp.int32)


def draw_choice_index(key, part):
    return draw_pair(key)[1].astype(jnp.int32)


def place_ends(values, rng, smallest, top_value):
    shape = values.shape
    index_at = [jax.random.randint(jax.random.fold_in(rng, axis), (), 0, shape[axis]) for axis in range(len(shape))]
    values = values.at[tuple(index_at)].set(smallest)
    longest = shape.index(max(shape))
    index_at[longest] = (index_at[longest] + 1) % shape[longest]
    return values.at[tuple(index_at)].set(top_value)


def shard_levels(stream_key, extent, shards, low, largest):
    level, own = 1.0, jax.random.fold_in(stream_key, 6)
    for position, parts in shards:
        draws = jnp.exp(jax.random.uniform(jax.random.fold_in(own, position), (parts,), jnp.float32, low / len(shards), largest / len(shards)))
        level = level * jnp.repeat(draws, extent[position] // parts).reshape([-1 if axis == position else 1 for axis in range(len(extent))])
    return level


def routed_block(own_key, own, number, rows, count, top, limit, skew):
    order = jax.random.permutation(own_key, count)
    packed, common = shares(count, rows * top, limit, skew, True), shares(count, rows * top, limit, skew, False)
    places = jnp.arange(count)

    def named(tallies, offset_by):
        used = int((tallies > 0).sum())
        fixed = max(1, used // 4)
        passed = fixed + (places - fixed + offset_by * (used - fixed)) % max(1, count - fixed)
        return jnp.zeros((count,), jnp.int32).at[order[jnp.where(places < fixed, places, passed)]].set(jnp.asarray(tallies, jnp.int32))

    tallies = jnp.where(number % 4 == 0, named(packed, number // 4), named(common, number - number // 4 - 1))
    mixed = jax.random.permutation(jax.random.fold_in(own, 3), count)
    giver, receiver = mixed[0:count // 2 * 2:2], mixed[1:count // 2 * 2:2]
    room = jnp.minimum(tallies[giver] - 1, limit - tallies[receiver]) // 2
    room = jnp.where((giver == order[0]) | (receiver == order[0]) | (tallies[receiver] == 0), 0, jnp.maximum(room, 0))
    passed = jax.random.randint(jax.random.fold_in(own, 4), (count // 2,), 0, 1 << 20) % (room + 1)
    tallies = tallies.at[giver].add(-passed).at[receiver].add(passed)
    items = jnp.searchsorted(jnp.cumsum(tallies), jnp.arange(rows * top), side="right").astype(jnp.int32)
    grid = items.reshape(top, rows).T
    grid = grid[jax.random.permutation(jax.random.fold_in(own, 1), rows)]
    offset_by = jax.random.randint(jax.random.fold_in(own, 2), (rows, 1), 0, top)
    return jnp.take_along_axis(grid, (jnp.arange(top)[None, :] + offset_by) % top, axis=1)


def shares(amount, total, limit, slope, full):
    portions = [(1 << 20) // math.isqrt(rank ** slope) + 1 for rank in range(1, amount + 1)]
    largest = limit if full else min(limit, max(-(-total // amount), total * portions[0] // sum(portions)))
    least = 1 if total - largest >= amount - 1 else 0
    counts, rest = [largest] + [least] * (amount - 1), total - largest - least * (amount - 1)
    while rest > 0:
        movable = [i for i in range(1, amount) if counts[i] < largest] or [i for i in range(1, amount) if counts[i] < limit]
        pool, budget = sum([portions[i] for i in movable]), rest
        for i in movable:
            extra = min(limit - counts[i], max(1, budget * portions[i] // pool), rest)
            counts[i] = counts[i] + extra
            rest = rest - extra
    return np.array(counts)


def noise(own_key, dims, deviation, bound, shards=(), kind=jnp.bfloat16):
    entries = jax.random.normal(own_key, dims, jnp.float32) * deviation
    if len(shards) > 0:
        entries = shard_levels(own_key, dims, shards, -0.22, 0.18) * entries
    return jnp.clip(entries, min=-bound, max=bound).astype(kind)


def setup_inputs(seed: int = 0) -> dict:
    splits = jax.random.split(jax.random.key(seed), 8)
    halo_rows = noise(splits[0], (SNAPS, HALOS, WIDTH), 1.0, 6.0, ((1, 128), (2, 2)))
    unmatched = place_ends((jax.random.randint(splits[1], (SNAPS, HALOS), 0, 3) < 2).astype(jnp.int32), jax.random.fold_in(splits[1], 1), 0, 1)
    owner_id_keys = jax.random.split(jax.random.fold_in(splits[2], 1), SNAPS * HALOS // HALO_DEV)
    owner_id_turns = jax.random.permutation(jax.random.fold_in(splits[2], 3), SNAPS * HALOS // HALO_DEV)
    owner_id = jax.vmap(lambda own, number: routed_block(jax.random.fold_in(splits[2], 2), own, number, HALO_DEV, N_SPACE, 1, CAP, 2))(owner_id_keys, owner_id_turns).reshape((SNAPS, HALOS, 1))
    cand_index = place_ends(jax.random.randint(splits[3], (SNAPS, HALOS, K), 0, CAND_DEV), jax.random.fold_in(splits[3], 1), 0, CAND_DEV - 1).astype(jnp.int32)
    lengths = draw_lengths(jax.random.fold_in(splits[7], 71), 0)
    choice_index = draw_choice_index(jax.random.fold_in(splits[7], 71), 0)
    desc_rows = noise(splits[6], (SNAPS, CANDS, WIDTH), 1.0, 6.0, ((1, 128), (2, 2)))
    return dict(halo_rows=halo_rows, unmatched=unmatched, owner_id=owner_id, cand_index=cand_index, lengths=lengths, choice_index=choice_index, desc_rows=desc_rows)


def reference(halo_rows, unmatched, owner_id, cand_index, lengths, choice_index, desc_rows):
    phantom_list = []
    best_list = []
    lane_ids = jnp.arange(K, dtype=jnp.int32)
    block_size = math.gcd(HALOS, 4096)
    for snapshot in range(SNAPS):
        rows_here = halo_rows[snapshot]
        desc_table = desc_rows[snapshot]
        glob = (owner_id[snapshot, :, 0][:, None] * CAND_DEV + cand_index[snapshot]).astype(jnp.int32)

        def score_block(pieces):
            rows_block, glob_block = pieces
            picked = desc_table[glob_block].astype(jnp.float32)
            return jnp.einsum('rkw,rw->rk', picked, rows_block.astype(jnp.float32))
        merit_full = lax.map(score_block, (rows_here.reshape(-1, block_size, WIDTH), glob.reshape(-1, block_size, K)))
        merit_full = merit_full.reshape(HALOS, K) / math.sqrt(WIDTH)
        live_halo = unmatched[snapshot] == 1
        used = lane_ids[None, :] < lengths[snapshot][:, None]
        live_entry = used & live_halo[:, None]
        quality = 1.0 + jax.nn.softplus(merit_full)
        claims = jnp.zeros((CANDS,), jnp.float32).at[glob.reshape(-1)].max(jnp.where(live_entry, quality, jnp.zeros_like(quality)).reshape(-1))
        pick_pos = choice_index[snapshot][:, None].astype(jnp.int32)
        chosen = jnp.take_along_axis(glob, pick_pos, 1)[:, 0]
        chosen_quality = jnp.take_along_axis(quality, pick_pos, 1)[:, 0]
        share_weight = chosen_quality / (chosen_quality + claims[chosen])
        blended = ((1.0 - share_weight)[:, None] * rows_here.astype(jnp.float32) + share_weight[:, None] * desc_table[chosen].astype(jnp.float32)).astype(jnp.bfloat16)
        phantom_list.append(jnp.where(live_halo[:, None], blended, rows_here))
        top_merit = lax.optimization_barrier(jnp.max(jnp.where(used, merit_full, jnp.full_like(merit_full, -1e+30)), axis=1))
        best_list.append(jnp.where(live_halo, top_merit, jnp.zeros_like(top_merit)).astype(jnp.bfloat16))
    return (jnp.stack(phantom_list), jnp.stack(best_list))
```

```python
import jax
import jax.numpy as jnp
from jax import lax
from jax.experimental import pallas as pl
from jax.experimental.pallas import tpu as pltpu
from jax.sharding import PartitionSpec as P

MESH = pl.DeviceIdType.MESH
PEERS = 128
HALOS = 128
CANDS = 512
SLOTS = 4
REQS = PEERS * SLOTS
HALF = 128
K = 16
ROWS = 16
NEG = -1e30
F32 = jnp.float32
BF16 = jnp.bfloat16


def iota(shape, dim):
    return lax.broadcasted_iota(jnp.int32, shape, dim)


def mm(a, b):
    return jnp.dot(a, b, preferred_element_type=F32)


def mm_nt(a, b):
    return lax.dot_general(a, b, (((1,), (1,)), ((), ())), preferred_element_type=F32)


def mm_tn(a, b):
    return lax.dot_general(a, b, (((0,), (0,)), ((), ())), preferred_element_type=F32)


def softplus(v):
    return jnp.maximum(v, 0.0) + jnp.log1p(jnp.exp(-jnp.abs(v)))


def drain(blocks, sem):
    most = blocks.at[pl.ds(0, blocks.shape[0] - 1)]
    pltpu.make_async_copy(most, most, sem).wait()


def kernel(
    halo_hbm, unm_hbm, own_hbm, cand_hbm, len_hbm, pick_hbm, desc_hbm,
    out_ref, best_ref,
    halo_v, unm_v, own_v, cand_v, len_v, pick_v, desc_v,
    send_v, recv_v, meta_s, meta_r, reply_v, back_v, bmeta_s, bmeta_r, bests,
    put_v, take_v, merit_v, picked_v, fields_v, res_v,
    load_sem, desc_sem, dsend, drecv, rsend, rrecv, msend, mrecv, psend, precv, bsend, brecv, xsend, xrecv, self_sem, pair_sem,
):
    me = lax.axis_index("space")
    core = lax.axis_index("rep")
    other = 1 - core
    mz, my, mx = me // 16, (me // 4) % 4, me % 4

    loads = [
        pltpu.make_async_copy(own_hbm, own_v, load_sem.at[0]),
        pltpu.make_async_copy(halo_hbm, halo_v, load_sem.at[1]),
        pltpu.make_async_copy(cand_hbm.at[pl.ds(2 * core, 2)], cand_v, load_sem.at[2]),
        pltpu.make_async_copy(unm_hbm, unm_v, load_sem.at[3]),
        pltpu.make_async_copy(len_hbm, len_v, load_sem.at[4]),
        pltpu.make_async_copy(pick_hbm, pick_v, load_sem.at[5]),
    ]
    for load in loads:
        load.start()
    desc_load = pltpu.make_async_copy(
        desc_hbm.at[pl.ds(2 * core, 2)], desc_v.at[core], desc_sem
    )
    desc_load.start()

    barrier = pltpu.get_barrier_semaphore()

    def peer(dz, dy, dx):
        return ((mz + dz) % 8) * 16 + ((my + dy) % 4) * 4 + (mx + dx) % 4

    for step in (4, 3, 5, 2, 6, 1, 7, 0):
        for dy in (2, 1, 3, 0):
            for dx in (2, 1, 3, 0):
                if step or dy or dx:
                    pl.semaphore_signal(
                        barrier, inc=1, device_id=(peer(step, dy, dx), core), device_id_type=MESH
                    )
                else:
                    pl.semaphore_signal(
                        barrier, inc=1, device_id=(me, other), device_id_type=MESH
                    )

    for load in loads:
        load.wait()

    lane_h = iota((HALOS, HALOS), 1)
    sub_h = iota((HALOS, HALOS), 0)
    before = (sub_h < lane_h).astype(BF16)
    owners = own_v[...]
    hots, goals, ranks = [], [], []
    for snap in range(4):
        owner = owners[snap : snap + 1, :]
        hot = (sub_h == owner).astype(F32)
        hot16 = hot.astype(BF16)
        rank = jnp.sum(mm(hot16, before) * hot, axis=0, keepdims=True)
        hots.append(hot16)
        ranks.append(rank)
        goals.append(owner.astype(F32) * 4.0 + 2.0 * (snap % 2) + rank)
    row_id = iota((REQS, 2 * HALOS), 0).astype(F32)
    for pair in range(2):
        goal = jnp.concatenate([goals[2 * pair], goals[2 * pair + 1]], axis=1)
        put = (row_id == goal).astype(F32).astype(BF16)
        rows = halo_v[2 * pair : 2 * pair + 2].reshape(2 * HALOS, HALF)
        send_v[pair * PEERS : (pair + 1) * PEERS] = mm(put, rows).astype(BF16).reshape(PEERS, SLOTS, HALF)
        put_v[pair] = put

    first = core == 0
    own_hot = [jnp.where(first, hots[j].astype(F32), hots[2 + j].astype(F32)) for j in range(2)]
    own_rank = [jnp.where(first, ranks[j], ranks[2 + j]) for j in range(2)]
    spans = len_v[...]
    picks = pick_v[...]
    lives = unm_v[...]
    folded = jnp.zeros((PEERS, HALF), F32)
    lane = iota((HALOS, HALF), 1)
    spread = (iota((K, HALF), 1) % 32 == iota((K, HALF), 0)).astype(BF16)
    lane_k = iota((HALOS, K), 1).astype(F32)
    for j in range(2):
        def mine(a):
            return jnp.where(first, a[j : j + 1, :], a[2 + j : 3 + j, :]).astype(F32)
        span = jnp.where(mine(lives) == 1.0, mine(spans), 0.0)
        pick = jnp.where(mine(lives) == 1.0, mine(picks), -1.0)
        slot = own_rank[j] + 2.0 * j
        rows8 = jnp.concatenate([span, pick, slot, jnp.zeros((HALOS - 3, HALOS), F32)], axis=0)
        cols = rows8.T
        span_c, pick_c, slot_c = cols[:, 0:1], cols[:, 1:2], cols[:, 2:3]
        listed = cand_v[j].astype(F32)
        coded = listed - jnp.where(listed < 256.0, 256.0, 255.0)
        chosen = jnp.sum(jnp.where(lane_k == pick_c, coded, 0.0), axis=1, keepdims=True)
        coded = jnp.where(lane_k < span_c, coded, 0.0)
        wide = mm(coded.astype(BF16), spread)
        wide = jnp.where(lane % 32 == K, chosen, wide)
        wide = jnp.where((lane // 32).astype(F32) == slot_c, wide, 0.0)
        folded = folded + mm(own_hot[j].astype(BF16), wide.astype(BF16))
    meta_s[...] = folded.reshape(PEERS, 1, HALF)

    pl.semaphore_wait(barrier, PEERS)
    pl.semaphore_signal(pair_sem, inc=1, device_id=(me, other), device_id_type=MESH)
    pl.semaphore_wait(pair_sem, 1)

    desc_send = pltpu.make_async_remote_copy(
        src_ref=desc_hbm.at[pl.ds(2 * other, 2)], dst_ref=desc_v.at[core],
        send_sem=dsend, recv_sem=drecv, device_id=(me, other), device_id_type=MESH,
    )
    desc_send.start()

    def send_requests(step, carry):
        far = 127 - step
        goal = peer(far // 16, (far // 4) % 4, far % 4)
        pltpu.make_async_remote_copy(
            src_ref=meta_s.at[goal], dst_ref=meta_r.at[me],
            send_sem=msend, recv_sem=mrecv, device_id=(goal, core), device_id_type=MESH,
        ).start()
        for pair in range(2):
            pltpu.make_async_remote_copy(
                src_ref=send_v.at[pair * PEERS + goal], dst_ref=recv_v.at[core * PEERS + me],
                send_sem=rsend, recv_sem=rrecv, device_id=(goal, pair), device_id_type=MESH,
            ).start()
        return carry

    lax.fori_loop(0, PEERS - 1, send_requests, 0)
    pltpu.make_async_remote_copy(
        src_ref=send_v.at[other * PEERS + me], dst_ref=recv_v.at[core * PEERS + me],
        send_sem=rsend, recv_sem=rrecv, device_id=(me, other), device_id_type=MESH,
    ).start()
    self_row = pltpu.make_async_copy(send_v.at[core * PEERS + me], recv_v.at[core * PEERS + me], self_sem.at[0])
    self_meta = pltpu.make_async_copy(meta_s.at[me], meta_r.at[me], self_sem.at[1])
    self_row.start()
    self_meta.start()

    col_id = iota((2 * HALOS, REQS), 1).astype(F32)
    for pair in range(2):
        goal_rows = jnp.concatenate(
            [goals[2 * pair], goals[2 * pair + 1], jnp.zeros((HALOS - 2, HALOS), F32)], axis=0
        )
        live_rows = jnp.concatenate(
            [lives[2 * pair : 2 * pair + 2, :].astype(F32), jnp.zeros((HALOS - 2, HALOS), F32)], axis=0
        )
        goal_c, live_c = goal_rows.T, live_rows.T
        goal_c = jnp.concatenate([goal_c[:, 0:1], goal_c[:, 1:2]], axis=0)
        live_c = jnp.concatenate([live_c[:, 0:1], live_c[:, 1:2]], axis=0)
        take_v[pair] = jnp.where((col_id == goal_c) & (live_c == 1.0), 1.0, 0.0).astype(BF16)

    desc_load.wait()
    desc_send.wait()
    self_row.wait()
    self_meta.wait()

    drain(meta_r, mrecv)
    copies = (((iota((REQS, PEERS), 0) // SLOTS) == iota((REQS, PEERS), 1))).astype(BF16)
    spreadm = mm(copies, meta_r[...].reshape(PEERS, HALF).astype(BF16))
    mine_lane = (iota((REQS, HALF), 1) // 32) == (iota((REQS, HALF), 0) % SLOTS)
    fold = (iota((HALF, HALF), 0) % 32 == iota((HALF, HALF), 1)).astype(BF16)
    fields_v[...] = mm(jnp.where(mine_lane, spreadm, 0.0).astype(BF16), fold)

    drain(recv_v, rrecv)
    rows = [recv_v[part * PEERS : (part + 1) * PEERS].reshape(REQS, HALF) for part in range(2)]
    odd = ((iota((REQS, HALF), 0) // 2) % 2).astype(F32)
    odd16 = odd.astype(BF16)
    even16 = (1.0 - odd).astype(BF16)
    left = jnp.concatenate(
        [rows[0] * even16, rows[1] * even16, rows[0] * odd16, rows[1] * odd16], axis=1
    )
    right = jnp.concatenate(
        [desc_v[0, 0], desc_v[1, 0], desc_v[0, 1], desc_v[1, 1]], axis=1
    )
    merit_v[...] = mm_nt(left, right) * 0.0625

    cid = iota((1, CANDS), 1)
    code = (cid - jnp.where(cid < 256, 256, 255)).astype(F32)
    lane_r = iota((ROWS, HALF), 1)

    def rows_pass(block, col):
        at = pl.ds(pl.multiple_of(block * ROWS, ROWS), ROWS)
        merit = merit_v[at, :]
        field = fields_v[at, :]
        kept = jnp.full((ROWS, CANDS), NEG, F32)
        for k in range(K):
            kept = jnp.where(field[:, k : k + 1] == code, merit, kept)
        pick = field[:, K : K + 1] == code
        picked_v[at, :] = jnp.where(pick, 1.0, 0.0).astype(BF16)
        top = jnp.max(kept, axis=1, keepdims=True)
        got = jnp.max(jnp.where(pick, merit, NEG), axis=1, keepdims=True)
        res_v[at, :] = jnp.where(lane_r == 0, top, got)
        return jnp.maximum(col, jnp.max(kept.reshape(ROWS // 8, 8, CANDS), axis=0))

    col = lax.fori_loop(0, REQS // ROWS, rows_pass, jnp.full((8, CANDS), NEG, F32))
    col = jnp.maximum(col, pltpu.roll(col, 4, 0))
    sub = iota((8, CANDS), 0)
    swapped = jnp.where(sub % 2 == 0, pltpu.roll(col, 7, 0), pltpu.roll(col, 1, 0))
    col = jnp.maximum(col, swapped)
    col = jnp.concatenate([col, col], axis=0)

    def claim_pass(block, carry):
        at = pl.ds(pl.multiple_of(block * ROWS, ROWS), ROWS)
        pick = picked_v[at, :].astype(F32) > 0.5
        claim = jnp.max(jnp.where(pick, col, NEG), axis=1, keepdims=True)
        res_v[at, :] = jnp.where(lane_r == 2, claim, res_v[at, :])
        return carry

    lax.fori_loop(0, REQS // ROWS, claim_pass, 0)

    res = res_v[...]
    quality = 1.0 + softplus(res)
    mine_q, claim_q = quality[:, 1:2], quality[:, 2:3]
    share = mine_q / (mine_q + claim_q)
    picked = picked_v[...]
    for part in range(2):
        even_rows = mm(picked, desc_v[part, 0])
        odd_rows = mm(picked, desc_v[part, 1])
        found = jnp.where(odd == 0.0, even_rows, odd_rows)
        blend = (1.0 - share) * rows[part].astype(F32) + share * found
        reply_v[part * PEERS : (part + 1) * PEERS] = blend.astype(BF16).reshape(PEERS, SLOTS, HALF)
    tops = jnp.where(iota((REQS, HALF), 1) == iota((REQS, HALF), 0) % SLOTS, res[:, 0:1], 0.0)
    bmeta_s[...] = mm_tn(copies, tops.astype(BF16)).reshape(PEERS, 1, HALF)

    def send_replies(step, carry):
        far = 127 - step
        goal = peer(far // 16, (far // 4) % 4, far % 4)
        pltpu.make_async_remote_copy(
            src_ref=bmeta_s.at[goal], dst_ref=bmeta_r.at[me],
            send_sem=bsend, recv_sem=brecv, device_id=(goal, core), device_id_type=MESH,
        ).start()
        for part in range(2):
            pltpu.make_async_remote_copy(
                src_ref=reply_v.at[part * PEERS + goal], dst_ref=back_v.at[core * PEERS + me],
                send_sem=psend, recv_sem=precv, device_id=(goal, part), device_id_type=MESH,
            ).start()
        return carry

    lax.fori_loop(0, PEERS - 1, send_replies, 0)
    pltpu.make_async_remote_copy(
        src_ref=reply_v.at[other * PEERS + me], dst_ref=back_v.at[core * PEERS + me],
        send_sem=psend, recv_sem=precv, device_id=(me, other), device_id_type=MESH,
    ).start()
    self_back = pltpu.make_async_copy(reply_v.at[core * PEERS + me], back_v.at[core * PEERS + me], self_sem.at[0])
    self_best = pltpu.make_async_copy(bmeta_s.at[me], bmeta_r.at[me], self_sem.at[1])
    self_back.start()
    self_best.start()
    self_best.wait()

    drain(bmeta_r, brecv)
    tops_back = bmeta_r[...].reshape(PEERS, HALF).astype(BF16)
    best_rows = []
    for j in range(2):
        found = mm_tn(tops_back, own_hot[j].astype(BF16))
        value = jnp.where(own_rank[j] == 0.0, found[2 * j : 2 * j + 1, :], found[2 * j + 1 : 2 * j + 2, :])
        live = jnp.where(first, lives[j : j + 1, :], lives[2 + j : 3 + j, :])
        best_rows.append(jnp.where(live == 1, value, 0.0))
    bests[core] = jnp.concatenate(best_rows + [jnp.zeros((6, HALOS), F32)], axis=0)
    best_send = pltpu.make_async_remote_copy(
        src_ref=bests.at[core], dst_ref=bests.at[core],
        send_sem=xsend, recv_sem=xrecv, device_id=(me, other), device_id_type=MESH,
    )
    best_send.start()

    self_back.wait()
    drain(back_v, precv)
    for pair in range(2):
        live_rows = jnp.concatenate(
            [lives[2 * pair : 2 * pair + 2, :].astype(F32), jnp.zeros((HALOS - 2, HALOS), F32)], axis=0
        ).T
        live_c = jnp.concatenate([live_rows[:, 0:1], live_rows[:, 1:2]], axis=0)
        came = mm(take_v[pair], back_v[pair * PEERS : (pair + 1) * PEERS].reshape(REQS, HALF))
        kept = halo_v[2 * pair : 2 * pair + 2].reshape(2 * HALOS, HALF).astype(F32)
        out = jnp.where(live_c == 1.0, came, kept)
        out_ref[2 * pair : 2 * pair + 2] = out.astype(BF16).reshape(2, HALOS, HALF)
    best_send.wait()
    best_ref[...] = jnp.concatenate([bests[0, 0:2], bests[1, 0:2]], axis=0).astype(BF16)

    drain(send_v, rsend)
    drain(reply_v, psend)
    drain(meta_s, msend)
    drain(bmeta_s, bsend)


def body(halo_rows, unmatched, owner_id, cand_index, lengths, choice_index, desc_rows):
    any_space = pl.BlockSpec(memory_space=pl.ANY)
    vmem = pl.BlockSpec(memory_space=pltpu.VMEM)
    dma = pltpu.SemaphoreType.DMA
    return pl.pallas_call(
        kernel,
        name="phantom",
        out_shape=(
            jax.ShapeDtypeStruct(halo_rows.shape, BF16),
            jax.ShapeDtypeStruct(unmatched.shape, BF16),
        ),
        in_specs=[any_space] * 7,
        out_specs=(vmem, vmem),
        scratch_shapes=[
            pltpu.VMEM((4, HALOS, HALF), BF16),
            pltpu.VMEM((4, HALOS), jnp.int32),
            pltpu.VMEM((4, HALOS), jnp.int32),
            pltpu.VMEM((2, HALOS, K), jnp.int32),
            pltpu.VMEM((4, HALOS), jnp.int32),
            pltpu.VMEM((4, HALOS), jnp.int32),
            pltpu.VMEM((2, 2, CANDS, HALF), BF16),
            pltpu.VMEM((2 * PEERS, SLOTS, HALF), BF16),
            pltpu.VMEM((2 * PEERS, SLOTS, HALF), BF16),
            pltpu.VMEM((PEERS, 1, HALF), F32),
            pltpu.VMEM((PEERS, 1, HALF), F32),
            pltpu.VMEM((2 * PEERS, SLOTS, HALF), BF16),
            pltpu.VMEM((2 * PEERS, SLOTS, HALF), BF16),
            pltpu.VMEM((PEERS, 1, HALF), F32),
            pltpu.VMEM((PEERS, 1, HALF), F32),
            pltpu.VMEM((2, 8, HALOS), F32),
            pltpu.VMEM((2, REQS, 2 * HALOS), BF16),
            pltpu.VMEM((2, 2 * HALOS, REQS), BF16),
            pltpu.VMEM((REQS, CANDS), F32),
            pltpu.VMEM((REQS, CANDS), BF16),
            pltpu.VMEM((REQS, HALF), F32),
            pltpu.VMEM((REQS, HALF), F32),
            dma((6,)), dma, dma, dma, dma, dma, dma, dma, dma, dma, dma, dma, dma, dma, dma((2,)),
            pltpu.SemaphoreType.REGULAR,
        ],
        compiler_params=pltpu.CompilerParams(collective_id=0, has_side_effects=True),
    )(halo_rows, unmatched, owner_id[:, :, 0], cand_index, lengths, choice_index, desc_rows)


def solution(mesh):
    in_specs = (
        P(None, "space", "rep"),
        P(None, "space"),
        P(None, "space", None),
        P(None, "space", None),
        P(None, "space"),
        P(None, "space"),
        P(None, "space", "rep"),
    )
    out_specs = (P(None, "space", "rep"), P(None, "space"))
    return jax.shard_map(body, mesh=mesh, in_specs=in_specs, out_specs=out_specs, check_vma=False)
```

```python
import jax
import jax.numpy as jnp
from jax import lax
from jax.experimental import pallas as pl
from jax.experimental.pallas import tpu as pltpu
from jax.sharding import PartitionSpec as P

MESH = pl.DeviceIdType.MESH
PEERS = 128
HALOS = 128
CANDS = 512
SLOTS = 4
REQS = PEERS * SLOTS
HALF = 128
K = 16
ROWS = 16
PLANE = 16 * SLOTS
NEG = -1e30
F32 = jnp.float32
BF16 = jnp.bfloat16


def iota(shape, dim):
    return lax.broadcasted_iota(jnp.int32, shape, dim)


def mm(a, b):
    return jnp.dot(a, b, preferred_element_type=F32)


def mm_nt(a, b):
    return lax.dot_general(a, b, (((1,), (1,)), ((), ())), preferred_element_type=F32)


def mm_tn(a, b):
    return lax.dot_general(a, b, (((0,), (0,)), ((), ())), preferred_element_type=F32)


def softplus(v):
    return jnp.maximum(v, 0.0) + jnp.log1p(jnp.exp(-jnp.abs(v)))


def drain(blocks, sem):
    most = blocks.at[pl.ds(0, blocks.shape[0] - 1)]
    pltpu.make_async_copy(most, most, sem).wait()


def kernel(
    halo_hbm, unm_hbm, own_hbm, cand_hbm, len_hbm, pick_hbm, desc_hbm,
    out_ref, best_ref,
    halo_v, unm_v, own_v, cand_v, len_v, pick_v, desc_v, right_v,
    send_v, recv_v, meta_s, meta_r, reply_v, back_v, bmeta_s, bmeta_r, bests,
    put_v, take_v, merit_v, picked_v, fields_v, res_v, found_v,
    load_sem, desc_sem, dsend, drecv, rsend, rrecv, msend, mrecv, psend, precv, bsend, brecv, xsend, xrecv, pair_sem,
):
    me = lax.axis_index("space")
    core = lax.axis_index("rep")
    other = 1 - core
    mz, my, mx = me // 16, (me // 4) % 4, me % 4

    loads = [
        pltpu.make_async_copy(own_hbm, own_v, load_sem.at[0]),
        pltpu.make_async_copy(halo_hbm, halo_v, load_sem.at[1]),
        pltpu.make_async_copy(cand_hbm.at[pl.ds(2 * core, 2)], cand_v, load_sem.at[2]),
        pltpu.make_async_copy(unm_hbm, unm_v, load_sem.at[3]),
        pltpu.make_async_copy(len_hbm, len_v, load_sem.at[4]),
        pltpu.make_async_copy(pick_hbm, pick_v, load_sem.at[5]),
    ]
    for load in loads:
        load.start()
    desc_load = pltpu.make_async_copy(
        desc_hbm.at[pl.ds(2 * core, 2)], desc_v.at[core], desc_sem
    )
    desc_load.start()

    barrier = pltpu.get_barrier_semaphore()
    in_plane = [((my + dy) % 4) * 4 + (mx + dx) % 4 for dy in (2, 1, 3, 0) for dx in (2, 1, 3, 0)]
    for dz in (4, 3, 5, 2, 6, 1, 7, 0):
        plane = ((mz + dz) % 8) * 16
        for spot in range(16):
            if dz or spot < 15:
                goal = (plane + in_plane[spot], core)
            else:
                goal = (me, other)
            pl.semaphore_signal(barrier, inc=1, device_id=goal, device_id_type=MESH)

    for load in loads:
        load.wait()

    lane_h = iota((HALOS, HALOS), 1)
    sub_h = iota((HALOS, HALOS), 0)
    before = (sub_h < lane_h).astype(BF16)
    owners = own_v[...]
    hots, goals, ranks = [], [], []
    for snap in range(4):
        owner = owners[snap : snap + 1, :]
        hot = (sub_h == owner).astype(F32)
        rank = jnp.sum(mm(hot.astype(BF16), before) * hot, axis=0, keepdims=True)
        hots.append(hot)
        ranks.append(rank)
        goals.append(owner.astype(F32) * 4.0 + 2.0 * (snap % 2) + rank)
    row_id = iota((REQS, 2 * HALOS), 0).astype(F32)
    for pair in range(2):
        goal = jnp.concatenate([goals[2 * pair], goals[2 * pair + 1]], axis=1)
        put = (row_id == goal).astype(F32).astype(BF16)
        rows = halo_v[2 * pair : 2 * pair + 2].reshape(2 * HALOS, HALF)
        send_v[pair * PEERS : (pair + 1) * PEERS] = mm(put, rows).astype(BF16).reshape(PEERS, SLOTS, HALF)

    first = core == 0
    own_hot = [jnp.where(first, hots[j], hots[2 + j]).astype(BF16) for j in range(2)]
    own_rank = [jnp.where(first, ranks[j], ranks[2 + j]) for j in range(2)]
    spans, picks, lives = len_v[...], pick_v[...], unm_v[...]
    folded = jnp.zeros((PEERS, HALF), F32)
    place = iota((K, HALOS), 0)
    for j in range(2):
        def mine(a):
            return jnp.where(first, a[j : j + 1, :], a[2 + j : 3 + j, :])
        span = jnp.where(mine(lives) == 1, mine(spans), 0)
        pick = jnp.where(mine(lives) == 1, mine(picks), -1)
        slot = own_rank[j] + 2.0 * j
        listed = cand_v[j]
        coded = (listed - jnp.where(listed < 256, 256, 255)).astype(F32)
        chosen = jnp.sum(jnp.where(place == pick, coded, 0.0), axis=0, keepdims=True)
        coded = jnp.where(place < span, coded, 0.0)
        tail = jnp.where(place == 0, chosen, 0.0)
        field = jnp.concatenate([coded, tail] * SLOTS, axis=0)
        field = jnp.where((sub_h // 32).astype(F32) == slot, field, 0.0)
        folded = folded + mm_nt(own_hot[j], field.astype(BF16))
    meta_s[...] = folded.reshape(PEERS, 1, HALF)

    pl.semaphore_wait(barrier, PEERS)
    pl.semaphore_signal(pair_sem, inc=1, device_id=(me, other), device_id_type=MESH)

    desc_send = pltpu.make_async_remote_copy(
        src_ref=desc_hbm.at[pl.ds(2 * other, 2)], dst_ref=desc_v.at[core],
        send_sem=dsend, recv_sem=drecv, device_id=(me, other), device_id_type=MESH,
    )
    desc_send.start()

    def reach(step):
        return 4 + (1 - 2 * (step % 2)) * ((step + 1) // 2)

    def remote(src, dst, send_sem, recv_sem, goal):
        pltpu.make_async_remote_copy(
            src_ref=src, dst_ref=dst, send_sem=send_sem, recv_sem=recv_sem,
            device_id=goal, device_id_type=MESH,
        ).start()

    def send_requests(step, carry):
        plane = ((mz + reach(step)) % 8) * 16
        for spot in range(15):
            goal = plane + in_plane[spot]
            remote(meta_s.at[goal], meta_r.at[me], msend, mrecv.at[step], (goal, core))
            remote(send_v.at[core * PEERS + goal], recv_v.at[core * PEERS + me], rsend, rrecv.at[step], (goal, core))

        @pl.when(step < 7)
        def _():
            goal = plane + in_plane[15]
            remote(meta_s.at[goal], meta_r.at[me], msend, mrecv.at[step], (goal, core))
            remote(send_v.at[core * PEERS + goal], recv_v.at[core * PEERS + me], rsend, rrecv.at[step], (goal, core))

        @pl.when(step == 0)
        def _():
            pl.semaphore_wait(pair_sem, 1)

        for spot in range(16):
            goal = plane + in_plane[spot]
            remote(send_v.at[other * PEERS + goal], recv_v.at[core * PEERS + me], rsend, rrecv.at[step], (goal, other))
        return carry

    lax.fori_loop(0, 8, send_requests, 0)
    self_row = pltpu.make_async_copy(send_v.at[core * PEERS + me], recv_v.at[core * PEERS + me], rrecv.at[7])
    self_meta = pltpu.make_async_copy(meta_s.at[me], meta_r.at[me], mrecv.at[7])
    self_row.start()
    self_meta.start()

    col_id = iota((2 * HALOS, REQS), 1).astype(F32)
    live_cols = []
    for pair in range(2):
        lists = jnp.concatenate(
            [goals[2 * pair], goals[2 * pair + 1], lives[2 * pair : 2 * pair + 2, :].astype(F32),
             jnp.zeros((HALOS - 4, HALOS), F32)], axis=0,
        ).T
        goal_c = jnp.concatenate([lists[:, 0:1], lists[:, 1:2]], axis=0)
        live_c = jnp.concatenate([lists[:, 2:3], lists[:, 3:4]], axis=0)
        take_v[pair] = jnp.where(col_id == goal_c, live_c, 0.0).astype(BF16)
        put_v[pair] = jnp.broadcast_to(live_c, (2 * HALOS, HALF))

    desc_load.wait()
    desc_send.wait()
    for snap in range(2):
        for part in range(2):
            right_v[(2 * snap + part) * HALF : (2 * snap + part + 1) * HALF, :] = desc_v[part, snap].T

    cid = iota((1, CANDS), 1)
    code = (cid - jnp.where(cid < 256, 256, 255)).astype(F32)
    lane_r = iota((ROWS, HALF), 1)
    odd = ((iota((PLANE, HALF), 0) // 2) % 2).astype(F32)
    odd16 = odd.astype(BF16)
    even16 = (1.0 - odd).astype(BF16)
    lane_p = iota((16, HALF), 1)

    def score_plane(step, col):
        back = ((mz + 8 - reach(step)) % 8) * 16
        base = pl.multiple_of(back * SLOTS, PLANE)
        at = pl.ds(base, PLANE)
        pltpu.make_async_copy(meta_r.at[pl.ds(0, 16)], meta_r.at[pl.ds(0, 16)], mrecv.at[step]).wait()
        got = meta_r[pl.ds(back, 16)].reshape(16, HALF)
        for slot in range(SLOTS):
            moved = got if slot == 0 else pltpu.roll(got, HALF - 32 * slot, 1)
            fields_v[pl.ds(base + slot, 16, stride=SLOTS), :] = moved
        pltpu.make_async_copy(recv_v.at[pl.ds(0, 32)], recv_v.at[pl.ds(0, 32)], rrecv.at[step]).wait()
        rows = [recv_v[pl.ds(part * PEERS + back, 16)].reshape(PLANE, HALF) for part in range(2)]
        left = jnp.concatenate(
            [rows[0] * even16, rows[1] * even16, rows[0] * odd16, rows[1] * odd16], axis=1
        )
        merit_v[...] = mm(left, right_v[...]) * 0.0625
        for block in range(PLANE // ROWS):
            here = pl.ds(block * ROWS, ROWS)
            there = pl.ds(pl.multiple_of(base + block * ROWS, ROWS), ROWS)
            merit = merit_v[here, :]
            field = fields_v[there, :]
            kept = jnp.full((ROWS, CANDS), NEG, F32)
            for k in range(K):
                kept = jnp.where(field[:, k : k + 1] == code, merit, kept)
            pick = field[:, K : K + 1] == code
            picked_v[there, :] = jnp.where(pick, 1.0, 0.0).astype(BF16)
            top = jnp.max(kept, axis=1, keepdims=True)
            got_merit = jnp.max(jnp.where(pick, merit, NEG), axis=1, keepdims=True)
            res_v[there, :] = jnp.where(lane_r < 64, top, got_merit)
            col = jnp.maximum(col, jnp.max(kept.reshape(ROWS // 8, 8, CANDS), axis=0))
        picked = picked_v[at, :]
        for part in range(2):
            even_rows = mm(picked, desc_v[part, 0])
            odd_rows = mm(picked, desc_v[part, 1])
            found_v[at, part * HALF : (part + 1) * HALF] = jnp.where(odd == 0.0, even_rows, odd_rows)
        tops = jnp.zeros((16, HALF), F32)
        for slot in range(SLOTS):
            tops = jnp.where(lane_p == slot, res_v[pl.ds(base + slot, 16, stride=SLOTS), :], tops)
        bmeta_s[pl.ds(back, 16)] = tops.reshape(16, 1, HALF)
        for spot in range(15):
            goal = back + in_plane[spot]
            remote(bmeta_s.at[goal], bmeta_r.at[me], bsend, brecv, (goal, core))

        @pl.when(step < 7)
        def _():
            goal = back + in_plane[15]
            remote(bmeta_s.at[goal], bmeta_r.at[me], bsend, brecv, (goal, core))

        return col

    col = lax.fori_loop(0, 8, score_plane, jnp.full((8, CANDS), NEG, F32))
    col = jnp.maximum(col, pltpu.roll(col, 4, 0))
    sub = iota((8, CANDS), 0)
    swapped = jnp.where(sub % 2 == 0, pltpu.roll(col, 7, 0), pltpu.roll(col, 1, 0))
    col = jnp.maximum(col, swapped)
    col = jnp.concatenate([col] * (PLANE // 8), axis=0)

    def reply_plane(step, carry):
        back = ((mz + 8 - reach(step)) % 8) * 16
        at = pl.ds(pl.multiple_of(back * SLOTS, PLANE), PLANE)
        pick = fields_v[at, :][:, K : K + 1] == code
        claim = jnp.max(jnp.where(pick, col, NEG), axis=1, keepdims=True)
        quality = 1.0 + softplus(jnp.where(iota((PLANE, HALF), 1) < 64, claim, res_v[at, :]))
        claim_q, mine_q = quality[:, 0:1], quality[:, 64:65]
        share = mine_q / (mine_q + claim_q)
        for part in range(2):
            blocks = pl.ds(part * PEERS + back, 16)
            row = recv_v[blocks].reshape(PLANE, HALF).astype(F32)
            blend = (1.0 - share) * row + share * found_v[at, part * HALF : (part + 1) * HALF]
            reply_v[blocks] = blend.astype(BF16).reshape(16, SLOTS, HALF)
        for spot in range(16):
            goal = back + in_plane[spot]
            remote(reply_v.at[other * PEERS + goal], back_v.at[core * PEERS + me], psend, precv, (goal, other))
        for spot in range(15):
            goal = back + in_plane[spot]
            remote(reply_v.at[core * PEERS + goal], back_v.at[core * PEERS + me], psend, precv, (goal, core))

        @pl.when(step < 7)
        def _():
            goal = back + in_plane[15]
            remote(reply_v.at[core * PEERS + goal], back_v.at[core * PEERS + me], psend, precv, (goal, core))

        return carry

    lax.fori_loop(0, 8, reply_plane, 0)
    self_back = pltpu.make_async_copy(reply_v.at[core * PEERS + me], back_v.at[core * PEERS + me], load_sem.at[0])
    self_best = pltpu.make_async_copy(bmeta_s.at[me], bmeta_r.at[me], load_sem.at[1])
    self_back.start()
    self_best.start()
    self_best.wait()
    drain(bmeta_r, brecv)
    tops_back = bmeta_r[...].reshape(PEERS, HALF).astype(BF16)
    best_rows = []
    for j in range(2):
        found = mm_tn(tops_back, own_hot[j])
        value = jnp.where(own_rank[j] == 0.0, found[2 * j : 2 * j + 1, :], found[2 * j + 1 : 2 * j + 2, :])
        live = jnp.where(first, lives[j : j + 1, :], lives[2 + j : 3 + j, :])
        best_rows.append(jnp.where(live == 1, value, 0.0))
    bests[core] = jnp.concatenate(best_rows + [jnp.zeros((6, HALOS), F32)], axis=0)
    best_send = pltpu.make_async_remote_copy(
        src_ref=bests.at[core], dst_ref=bests.at[core],
        send_sem=xsend, recv_sem=xrecv, device_id=(me, other), device_id_type=MESH,
    )
    best_send.start()
    drain(send_v, rsend)
    drain(meta_s, msend)
    drain(bmeta_s, bsend)
    best_send.wait()
    best_ref[...] = jnp.concatenate([bests[0, 0:2], bests[1, 0:2]], axis=0).astype(BF16)

    self_back.wait()
    drain(back_v, precv)
    for pair in range(2):
        came = mm(take_v[pair], back_v[pair * PEERS : (pair + 1) * PEERS].reshape(REQS, HALF))
        kept = halo_v[2 * pair : 2 * pair + 2].reshape(2 * HALOS, HALF).astype(F32)
        out = jnp.where(put_v[pair] == 1.0, came, kept)
        out_ref[2 * pair : 2 * pair + 2] = out.astype(BF16).reshape(2, HALOS, HALF)
    drain(reply_v, psend)


def body(halo_rows, unmatched, owner_id, cand_index, lengths, choice_index, desc_rows):
    any_space = pl.BlockSpec(memory_space=pl.ANY)
    vmem = pl.BlockSpec(memory_space=pltpu.VMEM)
    dma = pltpu.SemaphoreType.DMA
    return pl.pallas_call(
        kernel,
        name="phantom",
        out_shape=(
            jax.ShapeDtypeStruct(halo_rows.shape, BF16),
            jax.ShapeDtypeStruct(unmatched.shape, BF16),
        ),
        in_specs=[any_space] * 7,
        out_specs=(vmem, vmem),
        scratch_shapes=[
            pltpu.VMEM((4, HALOS, HALF), BF16),
            pltpu.VMEM((4, HALOS), jnp.int32),
            pltpu.VMEM((4, HALOS), jnp.int32),
            pltpu.VMEM((2, K, HALOS), jnp.int32),
            pltpu.VMEM((4, HALOS), jnp.int32),
            pltpu.VMEM((4, HALOS), jnp.int32),
            pltpu.VMEM((2, 2, CANDS, HALF), BF16),
            pltpu.VMEM((4 * HALF, CANDS), BF16),
            pltpu.VMEM((2 * PEERS, SLOTS, HALF), BF16),
            pltpu.VMEM((2 * PEERS, SLOTS, HALF), BF16),
            pltpu.VMEM((PEERS, 1, HALF), F32),
            pltpu.VMEM((PEERS, 1, HALF), F32),
            pltpu.VMEM((2 * PEERS, SLOTS, HALF), BF16),
            pltpu.VMEM((2 * PEERS, SLOTS, HALF), BF16),
            pltpu.VMEM((PEERS, 1, HALF), F32),
            pltpu.VMEM((PEERS, 1, HALF), F32),
            pltpu.VMEM((2, 8, HALOS), F32),
            pltpu.VMEM((2, 2 * HALOS, HALF), F32),
            pltpu.VMEM((2, 2 * HALOS, REQS), BF16),
            pltpu.VMEM((PLANE, CANDS), F32),
            pltpu.VMEM((REQS, CANDS), BF16),
            pltpu.VMEM((REQS, HALF), F32),
            pltpu.VMEM((REQS, HALF), F32),
            pltpu.VMEM((REQS, 2 * HALF), F32),
            dma((6,)), dma, dma, dma, dma, dma((8,)), dma, dma((8,)), dma, dma, dma, dma, dma, dma,
            pltpu.SemaphoreType.REGULAR,
        ],
        compiler_params=pltpu.CompilerParams(collective_id=0, has_side_effects=True),
    )(halo_rows, unmatched, owner_id[:, :, 0], jnp.swapaxes(cand_index, 1, 2), lengths, choice_index, desc_rows)


def solution(mesh):
    in_specs = (
        P(None, "space", "rep"),
        P(None, "space"),
        P(None, "space", None),
        P(None, "space", None),
        P(None, "space"),
        P(None, "space"),
        P(None, "space", "rep"),
    )
    out_specs = (P(None, "space", "rep"), P(None, "space"))
    return jax.shard_map(body, mesh=mesh, in_specs=in_specs, out_specs=out_specs, check_vma=False)
```

```python
import jax
import jax.numpy as jnp
from jax import lax
from jax.experimental import pallas as pl
from jax.experimental.pallas import tpu as pltpu
from jax.sharding import PartitionSpec as P

MESH = pl.DeviceIdType.MESH
PEERS = 128
HALOS = 128
CANDS = 512
SLOTS = 4
REQS = PEERS * SLOTS
HALF = 128
K = 16
ROWS = 16
PLANE = 16 * SLOTS
NEG = -1e30
F32 = jnp.float32
BF16 = jnp.bfloat16


def iota(shape, dim):
    return lax.broadcasted_iota(jnp.int32, shape, dim)


def mm(a, b):
    return jnp.dot(a, b, preferred_element_type=F32)


def mm_nt(a, b):
    return lax.dot_general(a, b, (((1,), (1,)), ((), ())), preferred_element_type=F32)


def mm_tn(a, b):
    return lax.dot_general(a, b, (((0,), (0,)), ((), ())), preferred_element_type=F32)


def softplus(v):
    return jnp.maximum(v, 0.0) + jnp.log1p(jnp.exp(-jnp.abs(v)))


def drain(blocks, sem):
    most = blocks.at[pl.ds(0, blocks.shape[0] - 1)]
    pltpu.make_async_copy(most, most, sem).wait()


def kernel(
    halo_hbm, unm_hbm, own_hbm, cand_hbm, len_hbm, pick_hbm, desc_hbm,
    out_ref, best_ref,
    halo_v, unm_v, own_v, cand_v, len_v, pick_v, desc_v, right_v,
    send_v, recv_v, meta_s, meta_r, reply_v, back_v, bmeta_s, bmeta_r, bests,
    put_v, take_v, merit_v, picked_v, fields_v, res_v, found_v, shut_v,
    load_sem, desc_sem, dsend, drecv, rsend, rrecv, msend, mrecv, psend, precv, bsend, brecv, xsend, xrecv, pair_sem,
):
    me = lax.axis_index("space")
    core = lax.axis_index("rep")
    other = 1 - core
    mz, my, mx = me // 16, (me // 4) % 4, me % 4

    loads = [
        pltpu.make_async_copy(own_hbm, own_v, load_sem.at[0]),
        pltpu.make_async_copy(halo_hbm, halo_v, load_sem.at[1]),
        pltpu.make_async_copy(cand_hbm.at[pl.ds(2 * core, 2)], cand_v, load_sem.at[2]),
        pltpu.make_async_copy(unm_hbm, unm_v, load_sem.at[3]),
        pltpu.make_async_copy(len_hbm, len_v, load_sem.at[4]),
        pltpu.make_async_copy(pick_hbm, pick_v, load_sem.at[5]),
    ]
    for load in loads:
        load.start()
    desc_load = pltpu.make_async_copy(
        desc_hbm.at[pl.ds(2 * core, 2)], desc_v.at[core], desc_sem
    )
    desc_load.start()

    barrier = pltpu.get_barrier_semaphore()
    in_plane = [((my + dy) % 4) * 4 + (mx + dx) % 4 for dy in (2, 1, 3, 0) for dx in (2, 1, 3, 0)]
    for dz in (4, 3, 5, 2, 6, 1, 7, 0):
        plane = ((mz + dz) % 8) * 16
        for spot in range(16):
            if dz or spot < 15:
                goal = (plane + in_plane[spot], core)
            else:
                goal = (me, other)
            pl.semaphore_signal(barrier, inc=1, device_id=goal, device_id_type=MESH)

    for load in loads:
        load.wait()

    lane_h = iota((HALOS, HALOS), 1)
    sub_h = iota((HALOS, HALOS), 0)
    before = (sub_h < lane_h).astype(BF16)
    owners = own_v[...]
    hots, goals, ranks = [], [], []
    for snap in range(4):
        owner = owners[snap : snap + 1, :]
        hot = (sub_h == owner).astype(F32)
        rank = jnp.sum(mm(hot.astype(BF16), before) * hot, axis=0, keepdims=True)
        hots.append(hot)
        ranks.append(rank)
        goals.append(owner.astype(F32) * 4.0 + 2.0 * (snap % 2) + rank)
    row_id = iota((REQS, 2 * HALOS), 0).astype(F32)
    for pair in range(2):
        goal = jnp.concatenate([goals[2 * pair], goals[2 * pair + 1]], axis=1)
        put = (row_id == goal).astype(F32).astype(BF16)
        rows = halo_v[2 * pair : 2 * pair + 2].reshape(2 * HALOS, HALF)
        send_v[pair * PEERS : (pair + 1) * PEERS] = mm(put, rows).astype(BF16).reshape(PEERS, SLOTS, HALF)

    first = core == 0
    own_hot = [jnp.where(first, hots[j], hots[2 + j]).astype(BF16) for j in range(2)]
    own_rank = [jnp.where(first, ranks[j], ranks[2 + j]) for j in range(2)]
    spans, picks, lives = len_v[...], pick_v[...], unm_v[...]
    folded = jnp.zeros((PEERS, HALF), F32)
    place = iota((K, HALOS), 0)
    for j in range(2):
        def mine(a):
            return jnp.where(first, a[j : j + 1, :], a[2 + j : 3 + j, :])
        span = jnp.where(mine(lives) == 1, mine(spans), 0)
        pick = jnp.where(mine(lives) == 1, mine(picks), -1)
        slot = own_rank[j] + 2.0 * j
        listed = cand_v[j]
        coded = (listed - jnp.where(listed < 256, 256, 255)).astype(F32)
        chosen = jnp.sum(jnp.where(place == pick, coded, 0.0), axis=0, keepdims=True)
        coded = jnp.where(place < span, coded, 0.0)
        tail = jnp.where(place == 0, chosen, 0.0)
        field = jnp.concatenate([coded, tail] * SLOTS, axis=0)
        field = jnp.where((sub_h // 32).astype(F32) == slot, field, 0.0)
        folded = folded + mm_nt(own_hot[j], field.astype(BF16))
    meta_s[...] = folded.reshape(PEERS, 1, HALF)

    pl.semaphore_wait(barrier, PEERS)
    pl.semaphore_signal(pair_sem, inc=1, device_id=(me, other), device_id_type=MESH)

    desc_send = pltpu.make_async_remote_copy(
        src_ref=desc_hbm.at[pl.ds(2 * other, 2)], dst_ref=desc_v.at[core],
        send_sem=dsend, recv_sem=drecv, device_id=(me, other), device_id_type=MESH,
    )
    desc_send.start()

    def reach(step):
        return 4 + (1 - 2 * (step % 2)) * ((step + 1) // 2)

    def remote(src, dst, send_sem, recv_sem, goal):
        pltpu.make_async_remote_copy(
            src_ref=src, dst_ref=dst, send_sem=send_sem, recv_sem=recv_sem,
            device_id=goal, device_id_type=MESH,
        ).start()

    def send_lists(step, carry):
        plane = ((mz + reach(step)) % 8) * 16
        for spot in range(15):
            goal = plane + in_plane[spot]
            remote(meta_s.at[goal], meta_r.at[me], msend, mrecv.at[step], (goal, core))

        @pl.when(step < 7)
        def _():
            goal = plane + in_plane[15]
            remote(meta_s.at[goal], meta_r.at[me], msend, mrecv.at[step], (goal, core))

        return carry

    def send_requests(step, carry):
        plane = ((mz + reach(step)) % 8) * 16
        for spot in range(15):
            goal = plane + in_plane[spot]
            remote(send_v.at[core * PEERS + goal], recv_v.at[core * PEERS + me], rsend, rrecv.at[step], (goal, core))

        @pl.when(step < 7)
        def _():
            goal = plane + in_plane[15]
            remote(send_v.at[core * PEERS + goal], recv_v.at[core * PEERS + me], rsend, rrecv.at[step], (goal, core))

        for spot in range(16):
            goal = plane + in_plane[spot]
            remote(send_v.at[other * PEERS + goal], recv_v.at[core * PEERS + me], rsend, rrecv.at[step], (goal, other))
        return carry

    lax.fori_loop(0, 8, send_lists, 0)
    pl.semaphore_wait(pair_sem, 1)
    lax.fori_loop(0, 8, send_requests, 0)
    self_row = pltpu.make_async_copy(send_v.at[core * PEERS + me], recv_v.at[core * PEERS + me], rrecv.at[7])
    self_meta = pltpu.make_async_copy(meta_s.at[me], meta_r.at[me], mrecv.at[7])
    self_row.start()
    self_meta.start()

    col_id = iota((2 * HALOS, REQS), 1).astype(F32)
    live_cols = []
    for pair in range(2):
        lists = jnp.concatenate(
            [goals[2 * pair], goals[2 * pair + 1], lives[2 * pair : 2 * pair + 2, :].astype(F32),
             jnp.zeros((HALOS - 4, HALOS), F32)], axis=0,
        ).T
        goal_c = jnp.concatenate([lists[:, 0:1], lists[:, 1:2]], axis=0)
        live_c = jnp.concatenate([lists[:, 2:3], lists[:, 3:4]], axis=0)
        take_v[pair] = jnp.where(col_id == goal_c, live_c, 0.0).astype(BF16)
        put_v[pair] = jnp.broadcast_to(live_c, (2 * HALOS, HALF))

    desc_load.wait()
    desc_send.wait()
    for snap in range(2):
        for part in range(2):
            right_v[(2 * snap + part) * HALF : (2 * snap + part + 1) * HALF, :] = desc_v[part, snap].T

    cid = iota((1, CANDS), 1)
    code = (cid - jnp.where(cid < 256, 256, 255)).astype(F32)
    lane_r = iota((ROWS, HALF), 1)
    odd = ((iota((PLANE, HALF), 0) // 2) % 2).astype(F32)
    odd16 = odd.astype(BF16)
    even16 = (1.0 - odd).astype(BF16)
    lane_p = iota((16, HALF), 1)

    def list_plane(turn, carry):
        step = 7 - turn
        back = ((mz + 8 - reach(step)) % 8) * 16
        base = pl.multiple_of(back * SLOTS, PLANE)
        at = pl.ds(base, PLANE)
        pltpu.make_async_copy(meta_r.at[pl.ds(0, 16)], meta_r.at[pl.ds(0, 16)], mrecv.at[step]).wait()
        got = meta_r[pl.ds(back, 16)].reshape(16, HALF)
        for slot in range(SLOTS):
            moved = got if slot == 0 else pltpu.roll(got, HALF - 32 * slot, 1)
            fields_v[pl.ds(base + slot, 16, stride=SLOTS), :] = moved
        for block in range(PLANE // ROWS):
            there = pl.ds(pl.multiple_of(base + block * ROWS, ROWS), ROWS)
            field = fields_v[there, :]
            shut = jnp.full((ROWS, CANDS), NEG, F32)
            for k in range(K):
                shut = jnp.where(field[:, k : k + 1] == code, 0.0, shut)
            shut_v[there, :] = shut
            pick = field[:, K : K + 1] == code
            picked_v[there, :] = jnp.where(pick, 1.0, 0.0).astype(BF16)
        picked = picked_v[at, :]
        for part in range(2):
            even_rows = mm(picked, desc_v[part, 0])
            odd_rows = mm(picked, desc_v[part, 1])
            found_v[at, part * HALF : (part + 1) * HALF] = jnp.where(odd == 0.0, even_rows, odd_rows)
        return carry

    lax.fori_loop(0, 8, list_plane, 0)

    def score_plane(step, col):
        back = ((mz + 8 - reach(step)) % 8) * 16
        base = pl.multiple_of(back * SLOTS, PLANE)
        at = pl.ds(base, PLANE)
        pltpu.make_async_copy(recv_v.at[pl.ds(0, 32)], recv_v.at[pl.ds(0, 32)], rrecv.at[step]).wait()
        rows = [recv_v[pl.ds(part * PEERS + back, 16)].reshape(PLANE, HALF) for part in range(2)]
        left = jnp.concatenate(
            [rows[0] * even16, rows[1] * even16, rows[0] * odd16, rows[1] * odd16], axis=1
        )
        merit_v[...] = mm(left, right_v[...])
        product = rows[0].astype(F32) * found_v[at, 0:HALF] + rows[1].astype(F32) * found_v[at, HALF : 2 * HALF]
        own_merit = jnp.sum(product, axis=1, keepdims=True)
        for block in range(PLANE // ROWS):
            here = pl.ds(block * ROWS, ROWS)
            there = pl.ds(pl.multiple_of(base + block * ROWS, ROWS), ROWS)
            kept = merit_v[here, :] + shut_v[there, :]
            top = jnp.max(kept, axis=1, keepdims=True)
            res_v[there, :] = jnp.where(lane_r < 64, top, own_merit[block * ROWS : (block + 1) * ROWS]) * 0.0625
            col = jnp.maximum(col, jnp.max(kept.reshape(ROWS // 8, 8, CANDS), axis=0))
        tops = jnp.zeros((16, HALF), F32)
        for slot in range(SLOTS):
            tops = jnp.where(lane_p == slot, res_v[pl.ds(base + slot, 16, stride=SLOTS), :], tops)
        bmeta_s[pl.ds(back, 16)] = tops.reshape(16, 1, HALF)
        for spot in range(15):
            goal = back + in_plane[spot]
            remote(bmeta_s.at[goal], bmeta_r.at[me], bsend, brecv, (goal, core))

        @pl.when(step < 7)
        def _():
            goal = back + in_plane[15]
            remote(bmeta_s.at[goal], bmeta_r.at[me], bsend, brecv, (goal, core))

        return col

    col = lax.fori_loop(0, 8, score_plane, jnp.full((8, CANDS), NEG, F32)) * 0.0625
    col = jnp.maximum(col, pltpu.roll(col, 4, 0))
    sub = iota((8, CANDS), 0)
    swapped = jnp.where(sub % 2 == 0, pltpu.roll(col, 7, 0), pltpu.roll(col, 1, 0))
    col = jnp.maximum(col, swapped)
    col = jnp.concatenate([col] * (PLANE // 8), axis=0)

    def reply_plane(step, carry):
        back = ((mz + 8 - reach(step)) % 8) * 16
        at = pl.ds(pl.multiple_of(back * SLOTS, PLANE), PLANE)
        pick = fields_v[at, :][:, K : K + 1] == code
        claim = jnp.max(jnp.where(pick, col, NEG), axis=1, keepdims=True)
        quality = 1.0 + softplus(jnp.where(iota((PLANE, HALF), 1) < 64, claim, res_v[at, :]))
        claim_q, mine_q = quality[:, 0:1], quality[:, 64:65]
        share = mine_q / (mine_q + claim_q)
        for part in range(2):
            blocks = pl.ds(part * PEERS + back, 16)
            row = recv_v[blocks].reshape(PLANE, HALF).astype(F32)
            blend = (1.0 - share) * row + share * found_v[at, part * HALF : (part + 1) * HALF]
            reply_v[blocks] = blend.astype(BF16).reshape(16, SLOTS, HALF)
        for spot in range(16):
            goal = back + in_plane[spot]
            remote(reply_v.at[other * PEERS + goal], back_v.at[core * PEERS + me], psend, precv, (goal, other))
        for spot in range(15):
            goal = back + in_plane[spot]
            remote(reply_v.at[core * PEERS + goal], back_v.at[core * PEERS + me], psend, precv, (goal, core))

        @pl.when(step < 7)
        def _():
            goal = back + in_plane[15]
            remote(reply_v.at[core * PEERS + goal], back_v.at[core * PEERS + me], psend, precv, (goal, core))

        return carry

    lax.fori_loop(0, 8, reply_plane, 0)
    self_back = pltpu.make_async_copy(reply_v.at[core * PEERS + me], back_v.at[core * PEERS + me], load_sem.at[0])
    self_best = pltpu.make_async_copy(bmeta_s.at[me], bmeta_r.at[me], load_sem.at[1])
    self_back.start()
    self_best.start()
    self_best.wait()
    drain(bmeta_r, brecv)
    tops_back = bmeta_r[...].reshape(PEERS, HALF).astype(BF16)
    best_rows = []
    for j in range(2):
        found = mm_tn(tops_back, own_hot[j])
        value = jnp.where(own_rank[j] == 0.0, found[2 * j : 2 * j + 1, :], found[2 * j + 1 : 2 * j + 2, :])
        live = jnp.where(first, lives[j : j + 1, :], lives[2 + j : 3 + j, :])
        best_rows.append(jnp.where(live == 1, value, 0.0))
    bests[core] = jnp.concatenate(best_rows + [jnp.zeros((6, HALOS), F32)], axis=0)
    best_send = pltpu.make_async_remote_copy(
        src_ref=bests.at[core], dst_ref=bests.at[core],
        send_sem=xsend, recv_sem=xrecv, device_id=(me, other), device_id_type=MESH,
    )
    best_send.start()
    drain(send_v, rsend)
    drain(meta_s, msend)
    drain(bmeta_s, bsend)
    best_send.wait()
    best_ref[...] = jnp.concatenate([bests[0, 0:2], bests[1, 0:2]], axis=0).astype(BF16)

    self_back.wait()
    drain(back_v, precv)
    for pair in range(2):
        came = mm(take_v[pair], back_v[pair * PEERS : (pair + 1) * PEERS].reshape(REQS, HALF))
        kept = halo_v[2 * pair : 2 * pair + 2].reshape(2 * HALOS, HALF).astype(F32)
        out = jnp.where(put_v[pair] == 1.0, came, kept)
        out_ref[2 * pair : 2 * pair + 2] = out.astype(BF16).reshape(2, HALOS, HALF)
    drain(reply_v, psend)


def body(halo_rows, unmatched, owner_id, cand_index, lengths, choice_index, desc_rows):
    any_space = pl.BlockSpec(memory_space=pl.ANY)
    vmem = pl.BlockSpec(memory_space=pltpu.VMEM)
    dma = pltpu.SemaphoreType.DMA
    return pl.pallas_call(
        kernel,
        name="phantom",
        out_shape=(
            pltpu.VMEM(halo_rows.shape, BF16),
            pltpu.VMEM(unmatched.shape, BF16),
        ),
        in_specs=[any_space] * 7,
        out_specs=(vmem, vmem),
        scratch_shapes=[
            pltpu.VMEM((4, HALOS, HALF), BF16),
            pltpu.VMEM((4, HALOS), jnp.int32),
            pltpu.VMEM((4, HALOS), jnp.int32),
            pltpu.VMEM((2, K, HALOS), jnp.int32),
            pltpu.VMEM((4, HALOS), jnp.int32),
            pltpu.VMEM((4, HALOS), jnp.int32),
            pltpu.VMEM((2, 2, CANDS, HALF), BF16),
            pltpu.VMEM((4 * HALF, CANDS), BF16),
            pltpu.VMEM((2 * PEERS, SLOTS, HALF), BF16),
            pltpu.VMEM((2 * PEERS, SLOTS, HALF), BF16),
            pltpu.VMEM((PEERS, 1, HALF), F32),
            pltpu.VMEM((PEERS, 1, HALF), F32),
            pltpu.VMEM((2 * PEERS, SLOTS, HALF), BF16),
            pltpu.VMEM((2 * PEERS, SLOTS, HALF), BF16),
            pltpu.VMEM((PEERS, 1, HALF), F32),
            pltpu.VMEM((PEERS, 1, HALF), F32),
            pltpu.VMEM((2, 8, HALOS), F32),
            pltpu.VMEM((2, 2 * HALOS, HALF), F32),
            pltpu.VMEM((2, 2 * HALOS, REQS), BF16),
            pltpu.VMEM((PLANE, CANDS), F32),
            pltpu.VMEM((REQS, CANDS), BF16),
            pltpu.VMEM((REQS, HALF), F32),
            pltpu.VMEM((REQS, HALF), F32),
            pltpu.VMEM((REQS, 2 * HALF), F32),
            pltpu.VMEM((REQS, CANDS), F32),
            dma((6,)), dma, dma, dma, dma, dma((8,)), dma, dma((8,)), dma, dma, dma, dma, dma, dma,
            pltpu.SemaphoreType.REGULAR,
        ],
        compiler_params=pltpu.CompilerParams(collective_id=0, has_side_effects=True),
    )(halo_rows, unmatched, owner_id[:, :, 0], jnp.swapaxes(cand_index, 1, 2), lengths, choice_index, desc_rows)


def solution(mesh):
    in_specs = (
        P(None, "space", "rep"),
        P(None, "space"),
        P(None, "space", None),
        P(None, "space", None),
        P(None, "space"),
        P(None, "space"),
        P(None, "space", "rep"),
    )
    out_specs = (P(None, "space", "rep"), P(None, "space"))
    return jax.shard_map(body, mesh=mesh, in_specs=in_specs, out_specs=out_specs, check_vma=False)
```

```python
import jax
import jax.numpy as jnp
from jax import lax
from jax.experimental import pallas as pl
from jax.experimental.pallas import tpu as pltpu
from jax.sharding import PartitionSpec as P

MESH = pl.DeviceIdType.MESH
PEERS = 128
HALOS = 128
CANDS = 512
SLOTS = 4
REQS = PEERS * SLOTS
HALF = 128
K = 16
ROWS = 16
PLANE = 16 * SLOTS
NEG = -1e30
F32 = jnp.float32
BF16 = jnp.bfloat16


def iota(shape, dim):
    return lax.broadcasted_iota(jnp.int32, shape, dim)


def mm(a, b):
    return jnp.dot(a, b, preferred_element_type=F32)


def mm_nt(a, b):
    return lax.dot_general(a, b, (((1,), (1,)), ((), ())), preferred_element_type=F32)


def mm_tn(a, b):
    return lax.dot_general(a, b, (((0,), (0,)), ((), ())), preferred_element_type=F32)


def softplus(v):
    return jnp.maximum(v, 0.0) + jnp.log1p(jnp.exp(-jnp.abs(v)))


def drain(blocks, sem):
    most = blocks.at[pl.ds(0, blocks.shape[0] - 1)]
    pltpu.make_async_copy(most, most, sem).wait()


def kernel(
    halo_hbm, unm_hbm, own_hbm, cand_hbm, len_hbm, pick_hbm, desc_hbm,
    out_ref, best_ref,
    halo_v, unm_v, own_v, cand_v, len_v, pick_v, desc_v, right_v,
    send_v, recv_v, meta_s, meta_r, reply_v, back_v, bmeta_s, bmeta_r, bests,
    put_v, take_v, merit_v, picked_v, fields_v, res_v, found_v, shut_v,
    load_sem, desc_sem, dsend, drecv, rsend, rrecv, msend, mrecv, psend, precv, bsend, brecv, xsend, xrecv, pair_sem, hsend, hrecv,
):
    me = lax.axis_index("space")
    core = lax.axis_index("rep")
    other = 1 - core
    mz, my, mx = me // 16, (me // 4) % 4, me % 4

    loads = [
        pltpu.make_async_copy(own_hbm, own_v, load_sem.at[0]),
        pltpu.make_async_copy(halo_hbm, halo_v, load_sem.at[1]),
        pltpu.make_async_copy(cand_hbm, cand_v, load_sem.at[2]),
        pltpu.make_async_copy(unm_hbm, unm_v, load_sem.at[3]),
        pltpu.make_async_copy(len_hbm, len_v, load_sem.at[4]),
        pltpu.make_async_copy(pick_hbm, pick_v, load_sem.at[5]),
    ]
    for load in loads:
        load.start()
    desc_load = pltpu.make_async_copy(
        desc_hbm.at[pl.ds(2 * core, 2)], desc_v.at[core], desc_sem
    )
    desc_load.start()

    barrier = pltpu.get_barrier_semaphore()
    in_plane = [((my + dy) % 4) * 4 + (mx + dx) % 4 for dy in (2, 1, 3, 0) for dx in (2, 1, 3, 0)]
    for dz in (4, 3, 5, 2, 6, 1, 7, 0):
        plane = ((mz + dz) % 8) * 16
        for spot in range(16):
            if dz or spot < 15:
                goal = (plane + in_plane[spot], core)
            else:
                goal = (me, other)
            pl.semaphore_signal(barrier, inc=1, device_id=goal, device_id_type=MESH)

    for load in loads:
        load.wait()

    lane_h = iota((HALOS, HALOS), 1)
    sub_h = iota((HALOS, HALOS), 0)
    before = (sub_h < lane_h).astype(BF16)
    owners = own_v[...]
    hots, goals, ranks = [], [], []
    for snap in range(4):
        owner = owners[snap : snap + 1, :]
        hot = (sub_h == owner).astype(F32)
        rank = jnp.sum(mm(hot.astype(BF16), before) * hot, axis=0, keepdims=True)
        hots.append(hot)
        ranks.append(rank)
        goals.append(owner.astype(F32) * 4.0 + 2.0 * (snap % 2) + rank)
    row_id = iota((REQS, 2 * HALOS), 0).astype(F32)
    for pair in range(2):
        goal = jnp.concatenate([goals[2 * pair], goals[2 * pair + 1]], axis=1)
        put = (row_id == goal).astype(F32).astype(BF16)
        rows = halo_v[2 * pair : 2 * pair + 2].reshape(2 * HALOS, HALF)
        send_v[pair * PEERS : (pair + 1) * PEERS] = mm(put, rows).astype(BF16).reshape(PEERS, SLOTS, HALF)

    first = core == 0
    own_hot = [jnp.where(first, hots[j], hots[2 + j]).astype(BF16) for j in range(2)]
    own_rank = [jnp.where(first, ranks[j], ranks[2 + j]) for j in range(2)]
    spans, picks, lives = len_v[...], pick_v[...], unm_v[...]
    folded = jnp.zeros((PEERS, HALF), F32)
    place = iota((K, HALOS), 0)
    for snap in range(4):
        row = slice(snap, snap + 1)
        span = jnp.where(lives[row] == 1, spans[row], 0)
        pick = picks[row]
        listed = cand_v[snap]
        coded = (listed - jnp.where(listed < 256, 256, 255)).astype(F32)
        chosen = jnp.sum(jnp.where(place == pick, coded, 0.0), axis=0, keepdims=True)
        coded = jnp.where(place == 0, chosen, jnp.where(place == pick, coded[0:1, :], coded))
        coded = jnp.where(place < span, coded, 0.0)
        field = jnp.concatenate([coded] * (2 * SLOTS), axis=0)
        slot = ranks[snap] + 2.0 * snap
        field = jnp.where((sub_h // K).astype(F32) == slot, field, 0.0)
        folded = folded + mm_nt(hots[snap].astype(BF16), field.astype(BF16))
    meta_s[...] = folded.reshape(PEERS, 1, HALF)

    pl.semaphore_wait(barrier, PEERS)
    pl.semaphore_signal(pair_sem, inc=1, device_id=(me, other), device_id_type=MESH)

    desc_send = pltpu.make_async_remote_copy(
        src_ref=desc_hbm.at[pl.ds(2 * other, 2)], dst_ref=desc_v.at[core],
        send_sem=dsend, recv_sem=drecv, device_id=(me, other), device_id_type=MESH,
    )
    desc_send.start()

    def reach(step):
        return 4 + (1 - 2 * (step % 2)) * ((step + 1) // 2)

    def mine_plane(turn):
        even = 4 + (1 - 2 * (turn % 2)) * (2 * ((turn + 1) // 2))
        odd = 4 - (1 - 2 * (turn % 2)) * (1 + 2 * (turn // 2))
        return even * other + odd * core

    def remote(src, dst, send_sem, recv_sem, goal):
        pltpu.make_async_remote_copy(
            src_ref=src, dst_ref=dst, send_sem=send_sem, recv_sem=recv_sem,
            device_id=goal, device_id_type=MESH,
        ).start()

    def send_lists(turn, carry):
        dz = mine_plane(turn)
        plane = ((mz + dz) % 8) * 16
        for spot in range(15):
            goal = plane + in_plane[spot]
            remote(meta_s.at[goal], meta_r.at[me], msend, mrecv.at[dz], (goal, core))

        @pl.when(dz > 0)
        def _():
            goal = plane + in_plane[15]
            remote(meta_s.at[goal], meta_r.at[me], msend, mrecv.at[dz], (goal, core))

        return carry

    def send_requests(step, carry):
        plane = ((mz + reach(step)) % 8) * 16
        for spot in range(15):
            goal = plane + in_plane[spot]
            remote(send_v.at[core * PEERS + goal], recv_v.at[core * PEERS + me], rsend, rrecv.at[reach(step)], (goal, core))

        @pl.when(step < 7)
        def _():
            goal = plane + in_plane[15]
            remote(send_v.at[core * PEERS + goal], recv_v.at[core * PEERS + me], rsend, rrecv.at[reach(step)], (goal, core))

        for spot in range(16):
            goal = plane + in_plane[spot]
            remote(send_v.at[other * PEERS + goal], recv_v.at[core * PEERS + me], rsend, rrecv.at[reach(step)], (goal, other))
        return carry

    lax.fori_loop(0, 4, send_lists, 0)
    pl.semaphore_wait(pair_sem, 1)
    lax.fori_loop(0, 8, send_requests, 0)
    self_row = pltpu.make_async_copy(send_v.at[core * PEERS + me], recv_v.at[core * PEERS + me], rrecv.at[0])
    self_row.start()

    @pl.when(core == 0)
    def _():
        pltpu.make_async_copy(meta_s.at[me], meta_r.at[me], mrecv.at[0]).start()

    col_id = iota((2 * HALOS, REQS), 1).astype(F32)
    live_cols = []
    for pair in range(2):
        lists = jnp.concatenate(
            [goals[2 * pair], goals[2 * pair + 1], lives[2 * pair : 2 * pair + 2, :].astype(F32),
             jnp.zeros((HALOS - 4, HALOS), F32)], axis=0,
        ).T
        goal_c = jnp.concatenate([lists[:, 0:1], lists[:, 1:2]], axis=0)
        live_c = jnp.concatenate([lists[:, 2:3], lists[:, 3:4]], axis=0)
        take_v[pair] = jnp.where(col_id == goal_c, live_c, 0.0).astype(BF16)
        put_v[pair] = jnp.broadcast_to(live_c, (2 * HALOS, HALF))

    desc_load.wait()
    desc_send.wait()
    for snap in range(2):
        for part in range(2):
            right_v[(2 * snap + part) * HALF : (2 * snap + part + 1) * HALF, :] = desc_v[part, snap].T

    cid = iota((1, CANDS), 1)
    code = (cid - jnp.where(cid < 256, 256, 255)).astype(F32)
    lane_r = iota((ROWS, HALF), 1)
    odd = ((iota((PLANE, HALF), 0) // 2) % 2).astype(F32)
    odd16 = odd.astype(BF16)
    even16 = (1.0 - odd).astype(BF16)
    lane_p = iota((16, HALF), 1)

    def hand_on(turn, carry):
        dz = mine_plane(3 - turn)
        back = ((mz + 8 - dz) % 8) * 16
        lists = meta_r.at[pl.ds(back, 16)]
        pltpu.make_async_copy(lists, lists, mrecv.at[dz]).wait()
        remote(lists, lists, hsend, hrecv.at[dz], (me, other))
        return carry

    lax.fori_loop(0, 4, hand_on, 0)

    def list_plane(turn, carry):
        step = 7 - turn
        back = ((mz + 8 - reach(step)) % 8) * 16
        base = pl.multiple_of(back * SLOTS, PLANE)
        at = pl.ds(base, PLANE)
        theirs = (reach(step) + core) % 2 == 1

        @pl.when(theirs)
        def _():
            pltpu.make_async_copy(meta_r.at[pl.ds(0, 16)], meta_r.at[pl.ds(0, 16)], hrecv.at[reach(step)]).wait()

        got = meta_r[pl.ds(back, 16)].reshape(16, HALF)
        for slot in range(SLOTS):
            shift = (HALF - K * slot) % HALF
            here = pltpu.roll(got, shift, 1) if slot else got
            moved = jnp.where(first, here, pltpu.roll(got, HALF // 2 - K * slot, 1))
            fields_v[pl.ds(base + slot, 16, stride=SLOTS), :] = moved
        for block in range(PLANE // ROWS):
            there = pl.ds(pl.multiple_of(base + block * ROWS, ROWS), ROWS)
            field = fields_v[there, :]
            shut = jnp.full((ROWS, CANDS), NEG, F32)
            for k in range(K):
                shut = jnp.where(field[:, k : k + 1] == code, 0.0, shut)
            shut_v[there, :] = shut
            pick = field[:, 0:1] == code
            picked_v[there, :] = jnp.where(pick, 1.0, 0.0).astype(BF16)
        picked = picked_v[at, :]
        for part in range(2):
            even_rows = mm(picked, desc_v[part, 0])
            odd_rows = mm(picked, desc_v[part, 1])
            found_v[at, part * HALF : (part + 1) * HALF] = jnp.where(odd == 0.0, even_rows, odd_rows)
        return carry

    lax.fori_loop(0, 8, list_plane, 0)

    def score_plane(step, col):
        back = ((mz + 8 - reach(step)) % 8) * 16
        base = pl.multiple_of(back * SLOTS, PLANE)
        at = pl.ds(base, PLANE)
        pltpu.make_async_copy(recv_v.at[pl.ds(0, 32)], recv_v.at[pl.ds(0, 32)], rrecv.at[reach(step)]).wait()
        rows = [recv_v[pl.ds(part * PEERS + back, 16)].reshape(PLANE, HALF) for part in range(2)]
        left = jnp.concatenate(
            [rows[0] * even16, rows[1] * even16, rows[0] * odd16, rows[1] * odd16], axis=1
        )
        merit_v[...] = mm(left, right_v[...])
        product = rows[0].astype(F32) * found_v[at, 0:HALF] + rows[1].astype(F32) * found_v[at, HALF : 2 * HALF]
        own_merit = jnp.sum(product, axis=1, keepdims=True)
        for block in range(PLANE // ROWS):
            here = pl.ds(block * ROWS, ROWS)
            there = pl.ds(pl.multiple_of(base + block * ROWS, ROWS), ROWS)
            kept = merit_v[here, :] + shut_v[there, :]
            top = jnp.max(kept, axis=1, keepdims=True)
            res_v[there, :] = jnp.where(lane_r < 64, top, own_merit[block * ROWS : (block + 1) * ROWS]) * 0.0625
            col = jnp.maximum(col, jnp.max(kept.reshape(ROWS // 8, 8, CANDS), axis=0))
        tops = jnp.zeros((16, HALF), F32)
        for slot in range(SLOTS):
            tops = jnp.where(lane_p == slot, res_v[pl.ds(base + slot, 16, stride=SLOTS), :], tops)
        bmeta_s[pl.ds(back, 16)] = tops.reshape(16, 1, HALF)
        for spot in range(15):
            goal = back + in_plane[spot]
            remote(bmeta_s.at[goal], bmeta_r.at[me], bsend, brecv, (goal, core))

        @pl.when(step < 7)
        def _():
            goal = back + in_plane[15]
            remote(bmeta_s.at[goal], bmeta_r.at[me], bsend, brecv, (goal, core))

        return col

    col = lax.fori_loop(0, 8, score_plane, jnp.full((8, CANDS), NEG, F32)) * 0.0625
    col = jnp.maximum(col, pltpu.roll(col, 4, 0))
    sub = iota((8, CANDS), 0)
    swapped = jnp.where(sub % 2 == 0, pltpu.roll(col, 7, 0), pltpu.roll(col, 1, 0))
    col = jnp.maximum(col, swapped)
    col = jnp.concatenate([col] * (PLANE // 8), axis=0)

    def reply_plane(step, carry):
        back = ((mz + 8 - reach(step)) % 8) * 16
        at = pl.ds(pl.multiple_of(back * SLOTS, PLANE), PLANE)
        pick = fields_v[at, :][:, 0:1] == code
        claim = jnp.max(jnp.where(pick, col, NEG), axis=1, keepdims=True)
        quality = 1.0 + softplus(jnp.where(iota((PLANE, HALF), 1) < 64, claim, res_v[at, :]))
        claim_q, mine_q = quality[:, 0:1], quality[:, 64:65]
        share = mine_q / (mine_q + claim_q)
        for part in range(2):
            blocks = pl.ds(part * PEERS + back, 16)
            row = recv_v[blocks].reshape(PLANE, HALF).astype(F32)
            blend = (1.0 - share) * row + share * found_v[at, part * HALF : (part + 1) * HALF]
            reply_v[blocks] = blend.astype(BF16).reshape(16, SLOTS, HALF)
        for spot in range(16):
            goal = back + in_plane[spot]
            remote(reply_v.at[other * PEERS + goal], back_v.at[core * PEERS + me], psend, precv, (goal, other))
        for spot in range(15):
            goal = back + in_plane[spot]
            remote(reply_v.at[core * PEERS + goal], back_v.at[core * PEERS + me], psend, precv, (goal, core))

        @pl.when(step < 7)
        def _():
            goal = back + in_plane[15]
            remote(reply_v.at[core * PEERS + goal], back_v.at[core * PEERS + me], psend, precv, (goal, core))

        return carry

    lax.fori_loop(0, 8, reply_plane, 0)
    self_back = pltpu.make_async_copy(reply_v.at[core * PEERS + me], back_v.at[core * PEERS + me], load_sem.at[0])
    self_best = pltpu.make_async_copy(bmeta_s.at[me], bmeta_r.at[me], load_sem.at[1])
    self_back.start()
    self_best.start()
    self_best.wait()
    drain(bmeta_r, brecv)
    tops_back = bmeta_r[...].reshape(PEERS, HALF).astype(BF16)
    best_rows = []
    for j in range(2):
        found = mm_tn(tops_back, own_hot[j])
        value = jnp.where(own_rank[j] == 0.0, found[2 * j : 2 * j + 1, :], found[2 * j + 1 : 2 * j + 2, :])
        live = jnp.where(first, lives[j : j + 1, :], lives[2 + j : 3 + j, :])
        best_rows.append(jnp.where(live == 1, value, 0.0))
    bests[core] = jnp.concatenate(best_rows + [jnp.zeros((6, HALOS), F32)], axis=0)
    best_send = pltpu.make_async_remote_copy(
        src_ref=bests.at[core], dst_ref=bests.at[core],
        send_sem=xsend, recv_sem=xrecv, device_id=(me, other), device_id_type=MESH,
    )
    best_send.start()
    drain(send_v, rsend)

    @pl.when(core == 0)
    def _():
        pltpu.make_async_copy(meta_s.at[pl.ds(0, 63)], meta_s.at[pl.ds(0, 63)], msend).wait()

    @pl.when(core == 1)
    def _():
        pltpu.make_async_copy(meta_s.at[pl.ds(0, 64)], meta_s.at[pl.ds(0, 64)], msend).wait()

    pltpu.make_async_copy(meta_s.at[pl.ds(0, 64)], meta_s.at[pl.ds(0, 64)], hsend).wait()
    drain(bmeta_s, bsend)
    best_send.wait()
    best_ref[...] = jnp.concatenate([bests[0, 0:2], bests[1, 0:2]], axis=0).astype(BF16)

    self_back.wait()
    drain(back_v, precv)
    for pair in range(2):
        came = mm(take_v[pair], back_v[pair * PEERS : (pair + 1) * PEERS].reshape(REQS, HALF))
        kept = halo_v[2 * pair : 2 * pair + 2].reshape(2 * HALOS, HALF).astype(F32)
        out = jnp.where(put_v[pair] == 1.0, came, kept)
        out_ref[2 * pair : 2 * pair + 2] = out.astype(BF16).reshape(2, HALOS, HALF)
    drain(reply_v, psend)


def write_out(out_v, best_v, out_hbm, best_hbm, sems):
    writes = [
        pltpu.make_async_copy(out_v, out_hbm, sems.at[0]),
        pltpu.make_async_copy(best_v, best_hbm, sems.at[1]),
    ]
    for write in writes:
        write.start()
    for write in writes:
        write.wait()


def body(halo_rows, unmatched, owner_id, cand_index, lengths, choice_index, desc_rows):
    any_space = pl.BlockSpec(memory_space=pl.ANY)
    vmem = pl.BlockSpec(memory_space=pltpu.VMEM)
    dma = pltpu.SemaphoreType.DMA
    out, best = pl.pallas_call(
        kernel,
        name="phantom",
        out_shape=(
            pltpu.VMEM(halo_rows.shape, BF16),
            pltpu.VMEM(unmatched.shape, BF16),
        ),
        in_specs=[any_space] * 7,
        out_specs=(vmem, vmem),
        scratch_shapes=[
            pltpu.VMEM((4, HALOS, HALF), BF16),
            pltpu.VMEM((4, HALOS), jnp.int32),
            pltpu.VMEM((4, HALOS), jnp.int32),
            pltpu.VMEM((4, K, HALOS), jnp.int32),
            pltpu.VMEM((4, HALOS), jnp.int32),
            pltpu.VMEM((4, HALOS), jnp.int32),
            pltpu.VMEM((2, 2, CANDS, HALF), BF16),
            pltpu.VMEM((4 * HALF, CANDS), BF16),
            pltpu.VMEM((2 * PEERS, SLOTS, HALF), BF16),
            pltpu.VMEM((2 * PEERS, SLOTS, HALF), BF16),
            pltpu.VMEM((PEERS, 1, HALF), F32),
            pltpu.VMEM((PEERS, 1, HALF), F32),
            pltpu.VMEM((2 * PEERS, SLOTS, HALF), BF16),
            pltpu.VMEM((2 * PEERS, SLOTS, HALF), BF16),
            pltpu.VMEM((PEERS, 1, HALF), F32),
            pltpu.VMEM((PEERS, 1, HALF), F32),
            pltpu.VMEM((2, 8, HALOS), F32),
            pltpu.VMEM((2, 2 * HALOS, HALF), F32),
            pltpu.VMEM((2, 2 * HALOS, REQS), BF16),
            pltpu.VMEM((PLANE, CANDS), F32),
            pltpu.VMEM((REQS, CANDS), BF16),
            pltpu.VMEM((REQS, HALF), F32),
            pltpu.VMEM((REQS, HALF), F32),
            pltpu.VMEM((REQS, 2 * HALF), F32),
            pltpu.VMEM((REQS, CANDS), F32),
            dma((6,)), dma, dma, dma, dma, dma((8,)), dma, dma((8,)), dma, dma, dma, dma, dma, dma,
            pltpu.SemaphoreType.REGULAR,
            dma, dma((8,)),
        ],
        compiler_params=pltpu.CompilerParams(collective_id=0, has_side_effects=True),
    )(halo_rows, unmatched, owner_id[:, :, 0], jnp.swapaxes(cand_index, 1, 2), lengths, choice_index, desc_rows)
    return pl.pallas_call(
        write_out,
        name="write",
        out_shape=(
            jax.ShapeDtypeStruct(halo_rows.shape, BF16),
            jax.ShapeDtypeStruct(unmatched.shape, BF16),
        ),
        in_specs=[vmem, vmem],
        out_specs=(any_space, any_space),
        scratch_shapes=[dma((2,))],
    )(pltpu.with_memory_space_constraint(out, pltpu.VMEM), pltpu.with_memory_space_constraint(best, pltpu.VMEM))


def solution(mesh):
    in_specs = (
        P(None, "space", "rep"),
        P(None, "space"),
        P(None, "space", None),
        P(None, "space", None),
        P(None, "space"),
        P(None, "space"),
        P(None, "space", "rep"),
    )
    out_specs = (P(None, "space", "rep"), P(None, "space"))
    return jax.shard_map(body, mesh=mesh, in_specs=in_specs, out_specs=out_specs, check_vma=False)
```

```python
import jax
import jax.numpy as jnp
from jax import lax
from jax.experimental import pallas as pl
from jax.experimental.pallas import tpu as pltpu
from jax.sharding import PartitionSpec as P

MESH = pl.DeviceIdType.MESH
PEERS = 128
HALOS = 128
CANDS = 512
SLOTS = 4
REQS = PEERS * SLOTS
HALF = 128
K = 16
ROWS = 16
PLANE = 16 * SLOTS
NEG = -1e30
F32 = jnp.float32
BF16 = jnp.bfloat16


def iota(shape, dim):
    return lax.broadcasted_iota(jnp.int32, shape, dim)


def mm(a, b):
    return jnp.dot(a, b, preferred_element_type=F32)


def mm_nt(a, b):
    return lax.dot_general(a, b, (((1,), (1,)), ((), ())), preferred_element_type=F32)


def mm_tn(a, b):
    return lax.dot_general(a, b, (((0,), (0,)), ((), ())), preferred_element_type=F32)


def softplus(v):
    return jnp.maximum(v, 0.0) + jnp.log1p(jnp.exp(-jnp.abs(v)))


def drain(blocks, sem):
    most = blocks.at[pl.ds(0, blocks.shape[0] - 1)]
    pltpu.make_async_copy(most, most, sem).wait()


def kernel(
    halo_hbm, unm_hbm, own_hbm, cand_hbm, len_hbm, pick_hbm, desc_hbm,
    out_ref, best_ref,
    halo_v, unm_v, own_v, cand_v, len_v, pick_v, desc_v, right_v,
    send_v, recv_v, meta_s, meta_r, reply_v, back_v, bmeta_s, bmeta_r,
    put_v, take_v, merit_v, picked_v, fields_v, res_v, found_v, shut_v, came_v,
    load_sem, desc_sem, dsend, drecv, rsend, rrecv, msend, mrecv, psend, precv, bsend, brecv, pair_sem, hsend, hrecv,
):
    me = lax.axis_index("space")
    core = lax.axis_index("rep")
    other = 1 - core
    mz, my, mx = me // 16, (me // 4) % 4, me % 4

    loads = [
        pltpu.make_async_copy(own_hbm, own_v, load_sem.at[0]),
        pltpu.make_async_copy(halo_hbm, halo_v, load_sem.at[1]),
        pltpu.make_async_copy(cand_hbm, cand_v, load_sem.at[2]),
        pltpu.make_async_copy(unm_hbm, unm_v, load_sem.at[3]),
        pltpu.make_async_copy(len_hbm, len_v, load_sem.at[4]),
        pltpu.make_async_copy(pick_hbm, pick_v, load_sem.at[5]),
    ]
    for load in loads:
        load.start()
    desc_load = pltpu.make_async_copy(
        desc_hbm.at[pl.ds(2 * core, 2)], desc_v.at[core], desc_sem
    )
    desc_load.start()

    barrier = pltpu.get_barrier_semaphore()
    in_plane = [((my + dy) % 4) * 4 + (mx + dx) % 4 for dy in (2, 1, 3, 0) for dx in (2, 1, 3, 0)]
    for dz in (4, 3, 5, 2, 6, 1, 7, 0):
        plane = ((mz + dz) % 8) * 16
        for spot in range(16):
            if dz or spot < 15:
                goal = (plane + in_plane[spot], core)
            else:
                goal = (me, other)
            pl.semaphore_signal(barrier, inc=1, device_id=goal, device_id_type=MESH)

    for load in loads:
        load.wait()

    lane_h = iota((HALOS, HALOS), 1)
    sub_h = iota((HALOS, HALOS), 0)
    before = (sub_h < lane_h).astype(BF16)
    owners = own_v[...]
    hots, goals, ranks = [], [], []
    for snap in range(4):
        owner = owners[snap : snap + 1, :]
        hot = (sub_h == owner).astype(F32)
        rank = jnp.sum(mm(hot.astype(BF16), before) * hot, axis=0, keepdims=True)
        hots.append(hot)
        ranks.append(rank)
        goals.append(owner.astype(F32) * 4.0 + 2.0 * (snap % 2) + rank)
    row_id = iota((REQS, 2 * HALOS), 0).astype(F32)
    for pair in range(2):
        goal = jnp.concatenate([goals[2 * pair], goals[2 * pair + 1]], axis=1)
        put = (row_id == goal).astype(F32).astype(BF16)
        rows = halo_v[2 * pair : 2 * pair + 2].reshape(2 * HALOS, HALF)
        send_v[pair * PEERS : (pair + 1) * PEERS] = mm(put, rows).astype(BF16).reshape(PEERS, SLOTS, HALF)

    first = core == 0
    own_hot = [jnp.where(first, hots[j], hots[2 + j]).astype(BF16) for j in range(2)]
    own_rank = [jnp.where(first, ranks[j], ranks[2 + j]) for j in range(2)]
    spans, picks, lives = len_v[...], pick_v[...], unm_v[...]
    folded = jnp.zeros((PEERS, HALF), F32)
    place = iota((K, HALOS), 0)
    for snap in range(4):
        row = slice(snap, snap + 1)
        span = jnp.where(lives[row] == 1, spans[row], 0)
        pick = picks[row]
        listed = cand_v[snap]
        coded = (listed - jnp.where(listed < 256, 256, 255)).astype(F32)
        chosen = jnp.sum(jnp.where(place == pick, coded, 0.0), axis=0, keepdims=True)
        coded = jnp.where(place == 0, chosen, jnp.where(place == pick, coded[0:1, :], coded))
        coded = jnp.where(place < span, coded, 0.0)
        field = jnp.concatenate([coded] * (2 * SLOTS), axis=0)
        slot = ranks[snap] + 2.0 * snap
        field = jnp.where((sub_h // K).astype(F32) == slot, field, 0.0)
        folded = folded + mm_nt(hots[snap].astype(BF16), field.astype(BF16))
    meta_s[...] = folded.reshape(PEERS, 1, HALF)

    pl.semaphore_wait(barrier, PEERS)
    pl.semaphore_signal(pair_sem, inc=1, device_id=(me, other), device_id_type=MESH)

    desc_send = pltpu.make_async_remote_copy(
        src_ref=desc_hbm.at[pl.ds(2 * other, 2)], dst_ref=desc_v.at[core],
        send_sem=dsend, recv_sem=drecv, device_id=(me, other), device_id_type=MESH,
    )
    desc_send.start()

    def reach(step):
        return 4 + (1 - 2 * (step % 2)) * ((step + 1) // 2)

    def mine_plane(turn):
        even = 4 + (1 - 2 * (turn % 2)) * (2 * ((turn + 1) // 2))
        odd = 4 - (1 - 2 * (turn % 2)) * (1 + 2 * (turn // 2))
        return even * other + odd * core

    def remote(src, dst, send_sem, recv_sem, goal):
        pltpu.make_async_remote_copy(
            src_ref=src, dst_ref=dst, send_sem=send_sem, recv_sem=recv_sem,
            device_id=goal, device_id_type=MESH,
        ).start()

    def send_lists(turn, carry):
        dz = mine_plane(turn)
        plane = ((mz + dz) % 8) * 16
        for spot in range(15):
            goal = plane + in_plane[spot]
            remote(meta_s.at[goal], meta_r.at[me], msend, mrecv.at[dz], (goal, core))

        @pl.when(dz > 0)
        def _():
            goal = plane + in_plane[15]
            remote(meta_s.at[goal], meta_r.at[me], msend, mrecv.at[dz], (goal, core))

        return carry

    def send_requests(step, carry):
        plane = ((mz + reach(step)) % 8) * 16
        for spot in range(15):
            goal = plane + in_plane[spot]
            remote(send_v.at[core * PEERS + goal], recv_v.at[core * PEERS + me], rsend, rrecv.at[reach(step)], (goal, core))

        @pl.when(step < 7)
        def _():
            goal = plane + in_plane[15]
            remote(send_v.at[core * PEERS + goal], recv_v.at[core * PEERS + me], rsend, rrecv.at[reach(step)], (goal, core))

        for spot in range(16):
            goal = plane + in_plane[spot]
            remote(send_v.at[other * PEERS + goal], recv_v.at[core * PEERS + me], rsend, rrecv.at[reach(step)], (goal, other))
        return carry

    lax.fori_loop(0, 4, send_lists, 0)
    pl.semaphore_wait(pair_sem, 1)
    lax.fori_loop(0, 8, send_requests, 0)
    self_row = pltpu.make_async_copy(send_v.at[core * PEERS + me], recv_v.at[core * PEERS + me], rrecv.at[0])
    self_row.start()

    @pl.when(core == 0)
    def _():
        pltpu.make_async_copy(meta_s.at[me], meta_r.at[me], mrecv.at[0]).start()

    col_id = iota((2 * HALOS, REQS), 1).astype(F32)
    live_cols = []
    for pair in range(2):
        lists = jnp.concatenate(
            [goals[2 * pair], goals[2 * pair + 1], lives[2 * pair : 2 * pair + 2, :].astype(F32),
             jnp.zeros((HALOS - 4, HALOS), F32)], axis=0,
        ).T
        goal_c = jnp.concatenate([lists[:, 0:1], lists[:, 1:2]], axis=0)
        live_c = jnp.concatenate([lists[:, 2:3], lists[:, 3:4]], axis=0)
        take_v[pair] = jnp.where(col_id == goal_c, live_c, 0.0).astype(BF16)
        put_v[pair] = jnp.broadcast_to(live_c, (2 * HALOS, HALF))

    desc_load.wait()
    desc_send.wait()
    for snap in range(2):
        for part in range(2):
            right_v[(2 * snap + part) * HALF : (2 * snap + part + 1) * HALF, :] = desc_v[part, snap].T

    cid = iota((1, CANDS), 1)
    code = (cid - jnp.where(cid < 256, 256, 255)).astype(F32)
    lane_r = iota((ROWS, HALF), 1)
    odd = ((iota((PLANE, HALF), 0) // 2) % 2).astype(F32)
    odd16 = odd.astype(BF16)
    even16 = (1.0 - odd).astype(BF16)
    lane_p = iota((16, HALF), 1)

    def hand_on(turn, carry):
        dz = mine_plane(3 - turn)
        back = ((mz + 8 - dz) % 8) * 16
        lists = meta_r.at[pl.ds(back, 16)]
        pltpu.make_async_copy(lists, lists, mrecv.at[dz]).wait()
        remote(lists, lists, hsend, hrecv.at[dz], (me, other))
        return carry

    lax.fori_loop(0, 4, hand_on, 0)

    def list_plane(turn, carry):
        step = 7 - turn
        back = ((mz + 8 - reach(step)) % 8) * 16
        base = pl.multiple_of(back * SLOTS, PLANE)
        at = pl.ds(base, PLANE)
        theirs = (reach(step) + core) % 2 == 1

        @pl.when(theirs)
        def _():
            pltpu.make_async_copy(meta_r.at[pl.ds(0, 16)], meta_r.at[pl.ds(0, 16)], hrecv.at[reach(step)]).wait()

        got = meta_r[pl.ds(back, 16)].reshape(16, HALF)
        for slot in range(SLOTS):
            shift = (HALF - K * slot) % HALF
            here = pltpu.roll(got, shift, 1) if slot else got
            moved = jnp.where(first, here, pltpu.roll(got, HALF // 2 - K * slot, 1))
            fields_v[pl.ds(base + slot, 16, stride=SLOTS), :] = moved
        for block in range(PLANE // ROWS):
            there = pl.ds(pl.multiple_of(base + block * ROWS, ROWS), ROWS)
            field = fields_v[there, :]
            shut = jnp.full((ROWS, CANDS), NEG, F32)
            for k in range(K):
                shut = jnp.where(field[:, k : k + 1] == code, 0.0, shut)
            shut_v[there, :] = shut
            pick = field[:, 0:1] == code
            picked_v[there, :] = jnp.where(pick, 1.0, 0.0).astype(BF16)
        picked = picked_v[at, :]
        for part in range(2):
            even_rows = mm(picked, desc_v[part, 0])
            odd_rows = mm(picked, desc_v[part, 1])
            found = jnp.where(odd == 0.0, even_rows, odd_rows)
            found_v[at, part * HALF : (part + 1) * HALF] = found
            reply_v[pl.ds(part * PEERS + back, 16)] = found.astype(BF16).reshape(16, SLOTS, HALF)
        for spot in range(16):
            goal = back + in_plane[spot]
            remote(reply_v.at[other * PEERS + goal], back_v.at[core * PEERS + me], psend, precv, (goal, other))
        for spot in range(15):
            goal = back + in_plane[spot]
            remote(reply_v.at[core * PEERS + goal], back_v.at[core * PEERS + me], psend, precv, (goal, core))

        @pl.when(step < 7)
        def _():
            goal = back + in_plane[15]
            remote(reply_v.at[core * PEERS + goal], back_v.at[core * PEERS + me], psend, precv, (goal, core))

        return carry

    lax.fori_loop(0, 8, list_plane, 0)
    self_back = pltpu.make_async_copy(reply_v.at[core * PEERS + me], back_v.at[core * PEERS + me], load_sem.at[0])
    self_back.start()

    def score_plane(step, col):
        back = ((mz + 8 - reach(step)) % 8) * 16
        base = pl.multiple_of(back * SLOTS, PLANE)
        at = pl.ds(base, PLANE)
        pltpu.make_async_copy(recv_v.at[pl.ds(0, 32)], recv_v.at[pl.ds(0, 32)], rrecv.at[reach(step)]).wait()
        rows = [recv_v[pl.ds(part * PEERS + back, 16)].reshape(PLANE, HALF) for part in range(2)]
        left = jnp.concatenate(
            [rows[0] * even16, rows[1] * even16, rows[0] * odd16, rows[1] * odd16], axis=1
        )
        merit_v[...] = mm(left, right_v[...])
        product = rows[0].astype(F32) * found_v[at, 0:HALF] + rows[1].astype(F32) * found_v[at, HALF : 2 * HALF]
        own_merit = jnp.sum(product, axis=1, keepdims=True)
        for block in range(PLANE // ROWS):
            here = pl.ds(block * ROWS, ROWS)
            there = pl.ds(pl.multiple_of(base + block * ROWS, ROWS), ROWS)
            kept = merit_v[here, :] + shut_v[there, :]
            top = jnp.max(kept, axis=1, keepdims=True)
            res_v[there, :] = jnp.where(lane_r < 64, top, own_merit[block * ROWS : (block + 1) * ROWS]) * 0.0625
            col = jnp.maximum(col, jnp.max(kept.reshape(ROWS // 8, 8, CANDS), axis=0))
        return col

    col = lax.fori_loop(0, 8, score_plane, jnp.full((8, CANDS), NEG, F32)) * 0.0625
    col = jnp.maximum(col, pltpu.roll(col, 4, 0))
    sub = iota((8, CANDS), 0)
    swapped = jnp.where(sub % 2 == 0, pltpu.roll(col, 7, 0), pltpu.roll(col, 1, 0))
    col = jnp.maximum(col, swapped)
    col = jnp.concatenate([col] * (PLANE // 8), axis=0)

    def reply_plane(step, carry):
        back = ((mz + 8 - reach(step)) % 8) * 16
        base = pl.multiple_of(back * SLOTS, PLANE)
        at = pl.ds(base, PLANE)
        top = res_v[at, :][:, 0:1]
        pick = fields_v[at, :][:, 0:1] == code
        claim = jnp.max(jnp.where(pick, col, NEG), axis=1, keepdims=True)
        quality = 1.0 + softplus(jnp.where(iota((PLANE, HALF), 1) < 64, claim, res_v[at, :]))
        claim_q, mine_q = quality[:, 0:1], quality[:, 64:65]
        share = mine_q / (mine_q + claim_q)
        res_v[at, :] = jnp.where(iota((PLANE, HALF), 1) < 64, share, top)
        tops = jnp.zeros((16, HALF), F32)
        for slot in range(SLOTS):
            tops = jnp.where(lane_p % 64 == slot, res_v[pl.ds(base + slot, 16, stride=SLOTS), :], tops)
        bmeta_s[pl.ds(back, 16)] = tops.reshape(16, 1, HALF)
        def news_to(spot, to):
            goal = back + in_plane[spot]
            remote(bmeta_s.at[goal], bmeta_r.at[core * PEERS + me], bsend, brecv, (goal, to))

        for spot in range(15):
            news_to(spot, core)
            news_to(spot, other)

        @pl.when(step < 7)
        def _():
            news_to(15, core)

        news_to(15, other)
        return carry

    lax.fori_loop(0, 8, reply_plane, 0)
    self_best = pltpu.make_async_copy(bmeta_s.at[me], bmeta_r.at[core * PEERS + me], load_sem.at[1])
    self_best.start()
    self_back.wait()
    drain(back_v, precv)
    for pair in range(2):
        came_v[pair] = mm(take_v[pair], back_v[pair * PEERS : (pair + 1) * PEERS].reshape(REQS, HALF))

    self_best.wait()
    drain(bmeta_r, brecv)
    best_rows = []
    for pair in range(2):
        news = bmeta_r[pair * PEERS : (pair + 1) * PEERS].reshape(PEERS, HALF)
        news_hi = news.astype(BF16)
        news_lo = (news - news_hi.astype(F32)).astype(BF16)
        share_rows = []
        for j in range(2):
            snap = 2 * pair + j
            hot = hots[snap].astype(BF16)
            coarse = mm_tn(news_hi, hot)
            fine = coarse + mm_tn(news_lo, hot)
            zero = ranks[snap] == 0.0
            best = jnp.where(zero, coarse[64 + 2 * j : 65 + 2 * j, :], coarse[65 + 2 * j : 66 + 2 * j, :])
            best_rows.append(jnp.where(lives[snap : snap + 1, :] == 1, best, 0.0))
            share_rows.append(jnp.where(zero, fine[2 * j : 2 * j + 1, :], fine[2 * j + 1 : 2 * j + 2, :]))
        cols = jnp.concatenate(share_rows + [jnp.zeros((HALOS - 2, HALOS), F32)], axis=0).T
        share = jnp.concatenate([cols[:, 0:1], cols[:, 1:2]], axis=0)
        kept = halo_v[2 * pair : 2 * pair + 2].reshape(2 * HALOS, HALF).astype(F32)
        blend = (1.0 - share) * kept + share * came_v[pair]
        out = jnp.where(put_v[pair] == 1.0, blend, kept)
        out_ref[2 * pair : 2 * pair + 2] = out.astype(BF16).reshape(2, HALOS, HALF)
    best_ref[...] = jnp.concatenate(best_rows, axis=0).astype(BF16)
    drain(send_v, rsend)

    @pl.when(core == 0)
    def _():
        pltpu.make_async_copy(meta_s.at[pl.ds(0, 63)], meta_s.at[pl.ds(0, 63)], msend).wait()

    @pl.when(core == 1)
    def _():
        pltpu.make_async_copy(meta_s.at[pl.ds(0, 64)], meta_s.at[pl.ds(0, 64)], msend).wait()

    pltpu.make_async_copy(meta_s.at[pl.ds(0, 64)], meta_s.at[pl.ds(0, 64)], hsend).wait()
    drain(bmeta_r, bsend)
    drain(reply_v, psend)


def write_out(out_v, best_v, out_hbm, best_hbm, sems):
    writes = [
        pltpu.make_async_copy(out_v, out_hbm, sems.at[0]),
        pltpu.make_async_copy(best_v, best_hbm, sems.at[1]),
    ]
    for write in writes:
        write.start()
    for write in writes:
        write.wait()


def body(halo_rows, unmatched, owner_id, cand_index, lengths, choice_index, desc_rows):
    any_space = pl.BlockSpec(memory_space=pl.ANY)
    vmem = pl.BlockSpec(memory_space=pltpu.VMEM)
    dma = pltpu.SemaphoreType.DMA
    out, best = pl.pallas_call(
        kernel,
        name="phantom",
        out_shape=(
            pltpu.VMEM(halo_rows.shape, BF16),
            pltpu.VMEM(unmatched.shape, BF16),
        ),
        in_specs=[any_space] * 7,
        out_specs=(vmem, vmem),
        scratch_shapes=[
            pltpu.VMEM((4, HALOS, HALF), BF16),
            pltpu.VMEM((4, HALOS), jnp.int32),
            pltpu.VMEM((4, HALOS), jnp.int32),
            pltpu.VMEM((4, K, HALOS), jnp.int32),
            pltpu.VMEM((4, HALOS), jnp.int32),
            pltpu.VMEM((4, HALOS), jnp.int32),
            pltpu.VMEM((2, 2, CANDS, HALF), BF16),
            pltpu.VMEM((4 * HALF, CANDS), BF16),
            pltpu.VMEM((2 * PEERS, SLOTS, HALF), BF16),
            pltpu.VMEM((2 * PEERS, SLOTS, HALF), BF16),
            pltpu.VMEM((PEERS, 1, HALF), F32),
            pltpu.VMEM((PEERS, 1, HALF), F32),
            pltpu.VMEM((2 * PEERS, SLOTS, HALF), BF16),
            pltpu.VMEM((2 * PEERS, SLOTS, HALF), BF16),
            pltpu.VMEM((PEERS, 1, HALF), F32),
            pltpu.VMEM((2 * PEERS, 1, HALF), F32),
            pltpu.VMEM((2, 2 * HALOS, HALF), F32),
            pltpu.VMEM((2, 2 * HALOS, REQS), BF16),
            pltpu.VMEM((PLANE, CANDS), F32),
            pltpu.VMEM((REQS, CANDS), BF16),
            pltpu.VMEM((REQS, HALF), F32),
            pltpu.VMEM((REQS, HALF), F32),
            pltpu.VMEM((REQS, 2 * HALF), F32),
            pltpu.VMEM((REQS, CANDS), F32),
            pltpu.VMEM((2, 2 * HALOS, HALF), F32),
            dma((6,)), dma, dma, dma, dma, dma((8,)), dma, dma((8,)), dma, dma, dma, dma,
            pltpu.SemaphoreType.REGULAR,
            dma, dma((8,)),
        ],
        compiler_params=pltpu.CompilerParams(collective_id=0, has_side_effects=True),
    )(halo_rows, unmatched, owner_id[:, :, 0], jnp.swapaxes(cand_index, 1, 2), lengths, choice_index, desc_rows)
    return pl.pallas_call(
        write_out,
        name="write",
        out_shape=(
            jax.ShapeDtypeStruct(halo_rows.shape, BF16),
            jax.ShapeDtypeStruct(unmatched.shape, BF16),
        ),
        in_specs=[vmem, vmem],
        out_specs=(any_space, any_space),
        scratch_shapes=[dma((2,))],
    )(pltpu.with_memory_space_constraint(out, pltpu.VMEM), pltpu.with_memory_space_constraint(best, pltpu.VMEM))


def solution(mesh):
    in_specs = (
        P(None, "space", "rep"),
        P(None, "space"),
        P(None, "space", None),
        P(None, "space", None),
        P(None, "space"),
        P(None, "space"),
        P(None, "space", "rep"),
    )
    out_specs = (P(None, "space", "rep"), P(None, "space"))
    return jax.shard_map(body, mesh=mesh, in_specs=in_specs, out_specs=out_specs, check_vma=False)
```

```python
import jax
import jax.numpy as jnp
from jax import lax
from jax.experimental import pallas as pl
from jax.experimental.pallas import tpu as pltpu
from jax.sharding import PartitionSpec as P

MESH = pl.DeviceIdType.MESH
PEERS = 128
HALOS = 128
CANDS = 512
SLOTS = 4
REQS = PEERS * SLOTS
HALF = 128
K = 16
ROWS = 16
PLANE = 16 * SLOTS
NEG = -1e30
F32 = jnp.float32
BF16 = jnp.bfloat16


def iota(shape, dim):
    return lax.broadcasted_iota(jnp.int32, shape, dim)


def mm(a, b):
    return jnp.dot(a, b, preferred_element_type=F32)


def mm_nt(a, b):
    return lax.dot_general(a, b, (((1,), (1,)), ((), ())), preferred_element_type=F32)


def mm_tn(a, b):
    return lax.dot_general(a, b, (((0,), (0,)), ((), ())), preferred_element_type=F32)


def softplus(v):
    return jnp.maximum(v, 0.0) + jnp.log1p(jnp.exp(-jnp.abs(v)))


def drain(blocks, sem):
    most = blocks.at[pl.ds(0, blocks.shape[0] - 1)]
    pltpu.make_async_copy(most, most, sem).wait()


def kernel(
    halo_hbm, unm_hbm, own_hbm, cand_hbm, len_hbm, pick_hbm, desc_hbm,
    out_ref, best_ref,
    halo_v, unm_v, own_v, cand_v, len_v, pick_v, desc_v, right_v,
    send_v, recv_v, meta_s, meta_r, reply_v, back_v, bmeta_s, bmeta_r,
    put_v, take_v, merit_v, picked_v, fields_v, res_v, found_v, shut_v, came_v,
    load_sem, desc_sem, dsend, drecv, rsend, rrecv, msend, mrecv, psend, precv, bsend, brecv, pair_sem, hsend, hrecv,
):
    me = lax.axis_index("space")
    core = lax.axis_index("rep")
    other = 1 - core
    mz, my, mx = me // 16, (me // 4) % 4, me % 4

    loads = [
        pltpu.make_async_copy(own_hbm, own_v, load_sem.at[0]),
        pltpu.make_async_copy(halo_hbm, halo_v, load_sem.at[1]),
        pltpu.make_async_copy(cand_hbm, cand_v, load_sem.at[2]),
        pltpu.make_async_copy(unm_hbm, unm_v, load_sem.at[3]),
        pltpu.make_async_copy(len_hbm, len_v, load_sem.at[4]),
        pltpu.make_async_copy(pick_hbm, pick_v, load_sem.at[5]),
    ]
    for load in loads:
        load.start()
    desc_load = pltpu.make_async_copy(
        desc_hbm.at[pl.ds(2 * core, 2)], desc_v.at[core], desc_sem
    )
    desc_load.start()

    barrier = pltpu.get_barrier_semaphore()
    in_plane = [((my + dy) % 4) * 4 + (mx + dx) % 4 for dy in (2, 1, 3, 0) for dx in (2, 1, 3, 0)]
    for dz in (4, 3, 5, 2, 6, 1, 7, 0):
        plane = ((mz + dz) % 8) * 16
        for spot in range(16):
            if dz or spot < 15:
                goal = (plane + in_plane[spot], core)
            else:
                goal = (me, other)
            pl.semaphore_signal(barrier, inc=1, device_id=goal, device_id_type=MESH)

    for load in loads:
        load.wait()

    lane_h = iota((HALOS, HALOS), 1)
    sub_h = iota((HALOS, HALOS), 0)
    before = (sub_h < lane_h).astype(BF16)
    owners = own_v[...]
    hots, goals, ranks = [], [], []
    for snap in range(4):
        owner = owners[snap : snap + 1, :]
        hot = (sub_h == owner).astype(F32)
        rank = jnp.sum(mm(hot.astype(BF16), before) * hot, axis=0, keepdims=True)
        hots.append(hot)
        ranks.append(rank)
        goals.append(owner.astype(F32) * 4.0 + 2.0 * (snap % 2) + rank)
    row_id = iota((REQS, 2 * HALOS), 0).astype(F32)
    for pair in range(2):
        goal = jnp.concatenate([goals[2 * pair], goals[2 * pair + 1]], axis=1)
        put = (row_id == goal).astype(F32).astype(BF16)
        rows = halo_v[2 * pair : 2 * pair + 2].reshape(2 * HALOS, HALF)
        send_v[pair * PEERS : (pair + 1) * PEERS] = mm(put, rows).astype(BF16).reshape(PEERS, SLOTS, HALF)

    first = core == 0
    own_hot = [jnp.where(first, hots[j], hots[2 + j]).astype(BF16) for j in range(2)]
    own_rank = [jnp.where(first, ranks[j], ranks[2 + j]) for j in range(2)]
    spans, picks, lives = len_v[...], pick_v[...], unm_v[...]
    folded = jnp.zeros((PEERS, HALF), F32)
    place = iota((K, HALOS), 0)
    for snap in range(4):
        row = slice(snap, snap + 1)
        span = jnp.where(lives[row] == 1, spans[row], 0)
        pick = picks[row]
        listed = cand_v[snap]
        coded = (listed - jnp.where(listed < 256, 256, 255)).astype(F32)
        chosen = jnp.sum(jnp.where(place == pick, coded, 0.0), axis=0, keepdims=True)
        coded = jnp.where(place == 0, chosen, jnp.where(place == pick, coded[0:1, :], coded))
        coded = jnp.where(place < span, coded, 0.0)
        field = jnp.concatenate([coded] * (2 * SLOTS), axis=0)
        slot = ranks[snap] + 2.0 * snap
        field = jnp.where((sub_h // K).astype(F32) == slot, field, 0.0)
        folded = folded + mm_nt(hots[snap].astype(BF16), field.astype(BF16))
    meta_s[...] = folded.reshape(PEERS, 1, HALF)

    pl.semaphore_wait(barrier, PEERS)
    pl.semaphore_signal(pair_sem, inc=1, device_id=(me, other), device_id_type=MESH)

    desc_send = pltpu.make_async_remote_copy(
        src_ref=desc_hbm.at[pl.ds(2 * other, 2)], dst_ref=desc_v.at[core],
        send_sem=dsend, recv_sem=drecv, device_id=(me, other), device_id_type=MESH,
    )
    desc_send.start()

    def reach(step):
        return 4 + (1 - 2 * (step % 2)) * ((step + 1) // 2)

    def mine_plane(turn):
        even = 4 + (1 - 2 * (turn % 2)) * (2 * ((turn + 1) // 2))
        odd = 4 - (1 - 2 * (turn % 2)) * (1 + 2 * (turn // 2))
        return even * other + odd * core

    def remote(src, dst, send_sem, recv_sem, goal):
        pltpu.make_async_remote_copy(
            src_ref=src, dst_ref=dst, send_sem=send_sem, recv_sem=recv_sem,
            device_id=goal, device_id_type=MESH,
        ).start()

    def send_lists(turn, carry):
        dz = mine_plane(turn)
        plane = ((mz + dz) % 8) * 16
        for spot in range(15):
            goal = plane + in_plane[spot]
            remote(meta_s.at[goal], meta_r.at[me], msend, mrecv.at[dz], (goal, core))

        @pl.when(dz > 0)
        def _():
            goal = plane + in_plane[15]
            remote(meta_s.at[goal], meta_r.at[me], msend, mrecv.at[dz], (goal, core))

        return carry

    def send_requests(step, carry):
        plane = ((mz + reach(step)) % 8) * 16

        def to_core(spot, to):
            goal = plane + in_plane[spot]
            remote(send_v.at[to * PEERS + goal], recv_v.at[core * PEERS + me], rsend, rrecv.at[reach(step)], (goal, to))

        for spot in range(15):
            to_core(spot, core)
            to_core(spot, other)

        @pl.when(step < 7)
        def _():
            to_core(15, core)

        to_core(15, other)
        return carry

    lax.fori_loop(0, 4, send_lists, 0)
    pl.semaphore_wait(pair_sem, 1)
    lax.fori_loop(0, 8, send_requests, 0)
    self_row = pltpu.make_async_copy(send_v.at[core * PEERS + me], recv_v.at[core * PEERS + me], rrecv.at[0])
    self_row.start()

    @pl.when(core == 0)
    def _():
        pltpu.make_async_copy(meta_s.at[me], meta_r.at[me], mrecv.at[0]).start()

    col_id = iota((2 * HALOS, REQS), 1).astype(F32)
    live_cols = []
    for pair in range(2):
        lists = jnp.concatenate(
            [goals[2 * pair], goals[2 * pair + 1], lives[2 * pair : 2 * pair + 2, :].astype(F32),
             jnp.zeros((HALOS - 4, HALOS), F32)], axis=0,
        ).T
        goal_c = jnp.concatenate([lists[:, 0:1], lists[:, 1:2]], axis=0)
        live_c = jnp.concatenate([lists[:, 2:3], lists[:, 3:4]], axis=0)
        take_v[pair] = jnp.where(col_id == goal_c, live_c, 0.0).astype(BF16)
        put_v[pair] = jnp.broadcast_to(live_c, (2 * HALOS, HALF))

    desc_load.wait()
    desc_send.wait()
    for snap in range(2):
        for part in range(2):
            right_v[(2 * snap + part) * HALF : (2 * snap + part + 1) * HALF, :] = desc_v[part, snap].T

    cid = iota((1, CANDS), 1)
    code = (cid - jnp.where(cid < 256, 256, 255)).astype(F32)
    lane_r = iota((ROWS, HALF), 1)
    odd = ((iota((PLANE, HALF), 0) // 2) % 2).astype(F32)
    odd16 = odd.astype(BF16)
    even16 = (1.0 - odd).astype(BF16)
    lane_p = iota((16, HALF), 1)

    def hand_on(turn, carry):
        dz = mine_plane(3 - turn)
        back = ((mz + 8 - dz) % 8) * 16
        lists = meta_r.at[pl.ds(back, 16)]
        pltpu.make_async_copy(lists, lists, mrecv.at[dz]).wait()
        remote(lists, lists, hsend, hrecv.at[dz], (me, other))
        return carry

    lax.fori_loop(0, 4, hand_on, 0)

    def list_plane(turn, carry):
        step = 7 - turn
        back = ((mz + 8 - reach(step)) % 8) * 16
        base = pl.multiple_of(back * SLOTS, PLANE)
        at = pl.ds(base, PLANE)
        theirs = (reach(step) + core) % 2 == 1

        @pl.when(theirs)
        def _():
            pltpu.make_async_copy(meta_r.at[pl.ds(0, 16)], meta_r.at[pl.ds(0, 16)], hrecv.at[reach(step)]).wait()

        got = meta_r[pl.ds(back, 16)].reshape(16, HALF)
        for slot in range(SLOTS):
            shift = (HALF - K * slot) % HALF
            here = pltpu.roll(got, shift, 1) if slot else got
            moved = jnp.where(first, here, pltpu.roll(got, HALF // 2 - K * slot, 1))
            fields_v[pl.ds(base + slot, 16, stride=SLOTS), :] = moved
        for block in range(PLANE // ROWS):
            there = pl.ds(pl.multiple_of(base + block * ROWS, ROWS), ROWS)
            field = fields_v[there, :]
            shut = jnp.full((ROWS, CANDS), NEG, F32)
            for k in range(K):
                shut = jnp.where(field[:, k : k + 1] == code, 0.0, shut)
            shut_v[there, :] = shut
            pick = field[:, 0:1] == code
            picked_v[there, :] = jnp.where(pick, 1.0, 0.0).astype(BF16)
        picked = picked_v[at, :]
        for part in range(2):
            even_rows = mm(picked, desc_v[part, 0])
            odd_rows = mm(picked, desc_v[part, 1])
            found = jnp.where(odd == 0.0, even_rows, odd_rows)
            found_v[at, part * HALF : (part + 1) * HALF] = found
            reply_v[pl.ds(part * PEERS + back, 16)] = found.astype(BF16).reshape(16, SLOTS, HALF)
        def row_to(spot, to):
            goal = back + in_plane[spot]
            remote(reply_v.at[to * PEERS + goal], back_v.at[core * PEERS + me], psend, precv, (goal, to))

        for spot in range(15):
            row_to(spot, core)
            row_to(spot, other)

        @pl.when(step < 7)
        def _():
            row_to(15, core)

        row_to(15, other)
        return carry

    lax.fori_loop(0, 8, list_plane, 0)
    self_back = pltpu.make_async_copy(reply_v.at[core * PEERS + me], back_v.at[core * PEERS + me], load_sem.at[0])
    self_back.start()

    def score_plane(step, col):
        back = ((mz + 8 - reach(step)) % 8) * 16
        base = pl.multiple_of(back * SLOTS, PLANE)
        at = pl.ds(base, PLANE)
        pltpu.make_async_copy(recv_v.at[pl.ds(0, 32)], recv_v.at[pl.ds(0, 32)], rrecv.at[reach(step)]).wait()
        rows = [recv_v[pl.ds(part * PEERS + back, 16)].reshape(PLANE, HALF) for part in range(2)]
        left = jnp.concatenate(
            [rows[0] * even16, rows[1] * even16, rows[0] * odd16, rows[1] * odd16], axis=1
        )
        merit_v[...] = mm(left, right_v[...])
        product = rows[0].astype(F32) * found_v[at, 0:HALF] + rows[1].astype(F32) * found_v[at, HALF : 2 * HALF]
        own_merit = jnp.sum(product, axis=1, keepdims=True)
        for block in range(PLANE // ROWS):
            here = pl.ds(block * ROWS, ROWS)
            there = pl.ds(pl.multiple_of(base + block * ROWS, ROWS), ROWS)
            kept = merit_v[here, :] + shut_v[there, :]
            top = jnp.max(kept, axis=1, keepdims=True)
            res_v[there, :] = jnp.where(lane_r < 64, top, own_merit[block * ROWS : (block + 1) * ROWS]) * 0.0625
            col = jnp.maximum(col, jnp.max(kept.reshape(ROWS // 8, 8, CANDS), axis=0))
        return col

    col = lax.fori_loop(0, 8, score_plane, jnp.full((8, CANDS), NEG, F32)) * 0.0625
    col = jnp.maximum(col, pltpu.roll(col, 4, 0))
    sub = iota((8, CANDS), 0)
    swapped = jnp.where(sub % 2 == 0, pltpu.roll(col, 7, 0), pltpu.roll(col, 1, 0))
    col = jnp.maximum(col, swapped)
    col = jnp.concatenate([col] * (PLANE // 8), axis=0)

    def reply_plane(step, carry):
        back = ((mz + 8 - reach(step)) % 8) * 16
        base = pl.multiple_of(back * SLOTS, PLANE)
        at = pl.ds(base, PLANE)
        top = res_v[at, :][:, 0:1]
        pick = fields_v[at, :][:, 0:1] == code
        claim = jnp.max(jnp.where(pick, col, NEG), axis=1, keepdims=True)
        quality = 1.0 + softplus(jnp.where(iota((PLANE, HALF), 1) < 64, claim, res_v[at, :]))
        claim_q, mine_q = quality[:, 0:1], quality[:, 64:65]
        share = mine_q / (mine_q + claim_q)
        res_v[at, :] = jnp.where(iota((PLANE, HALF), 1) < 64, share, top)
        tops = jnp.zeros((16, HALF), F32)
        for slot in range(SLOTS):
            tops = jnp.where(lane_p % 64 == slot, res_v[pl.ds(base + slot, 16, stride=SLOTS), :], tops)
        bmeta_s[pl.ds(back, 16)] = tops.reshape(16, 1, HALF)
        def news_to(spot, to):
            goal = back + in_plane[spot]
            remote(bmeta_s.at[goal], bmeta_r.at[core * PEERS + me], bsend, brecv, (goal, to))

        for spot in range(15):
            news_to(spot, core)
            news_to(spot, other)

        @pl.when(step < 7)
        def _():
            news_to(15, core)

        news_to(15, other)
        return carry

    lax.fori_loop(0, 8, reply_plane, 0)
    self_best = pltpu.make_async_copy(bmeta_s.at[me], bmeta_r.at[core * PEERS + me], load_sem.at[1])
    self_best.start()
    self_back.wait()
    drain(back_v, precv)
    for pair in range(2):
        came_v[pair] = mm(take_v[pair], back_v[pair * PEERS : (pair + 1) * PEERS].reshape(REQS, HALF))

    self_best.wait()
    drain(bmeta_r, brecv)
    best_rows = []
    for pair in range(2):
        news = bmeta_r[pair * PEERS : (pair + 1) * PEERS].reshape(PEERS, HALF)
        news_hi = news.astype(BF16)
        news_lo = (news - news_hi.astype(F32)).astype(BF16)
        share_rows = []
        for j in range(2):
            snap = 2 * pair + j
            hot = hots[snap].astype(BF16)
            coarse = mm_tn(news_hi, hot)
            fine = coarse + mm_tn(news_lo, hot)
            zero = ranks[snap] == 0.0
            best = jnp.where(zero, coarse[64 + 2 * j : 65 + 2 * j, :], coarse[65 + 2 * j : 66 + 2 * j, :])
            best_rows.append(jnp.where(lives[snap : snap + 1, :] == 1, best, 0.0))
            share_rows.append(jnp.where(zero, fine[2 * j : 2 * j + 1, :], fine[2 * j + 1 : 2 * j + 2, :]))
        cols = jnp.concatenate(share_rows + [jnp.zeros((HALOS - 2, HALOS), F32)], axis=0).T
        share = jnp.concatenate([cols[:, 0:1], cols[:, 1:2]], axis=0)
        kept = halo_v[2 * pair : 2 * pair + 2].reshape(2 * HALOS, HALF).astype(F32)
        blend = (1.0 - share) * kept + share * came_v[pair]
        out = jnp.where(put_v[pair] == 1.0, blend, kept)
        out_ref[2 * pair : 2 * pair + 2] = out.astype(BF16).reshape(2, HALOS, HALF)
    best_ref[...] = jnp.concatenate(best_rows, axis=0).astype(BF16)
    drain(send_v, rsend)

    @pl.when(core == 0)
    def _():
        pltpu.make_async_copy(meta_s.at[pl.ds(0, 63)], meta_s.at[pl.ds(0, 63)], msend).wait()

    @pl.when(core == 1)
    def _():
        pltpu.make_async_copy(meta_s.at[pl.ds(0, 64)], meta_s.at[pl.ds(0, 64)], msend).wait()

    pltpu.make_async_copy(meta_s.at[pl.ds(0, 64)], meta_s.at[pl.ds(0, 64)], hsend).wait()
    drain(bmeta_r, bsend)
    drain(reply_v, psend)


def write_out(out_v, best_v, out_hbm, best_hbm, sems):
    writes = [
        pltpu.make_async_copy(out_v, out_hbm, sems.at[0]),
        pltpu.make_async_copy(best_v, best_hbm, sems.at[1]),
    ]
    for write in writes:
        write.start()
    for write in writes:
        write.wait()


def body(halo_rows, unmatched, owner_id, cand_index, lengths, choice_index, desc_rows):
    any_space = pl.BlockSpec(memory_space=pl.ANY)
    vmem = pl.BlockSpec(memory_space=pltpu.VMEM)
    dma = pltpu.SemaphoreType.DMA
    out, best = pl.pallas_call(
        kernel,
        name="phantom",
        out_shape=(
            pltpu.VMEM(halo_rows.shape, BF16),
            pltpu.VMEM(unmatched.shape, BF16),
        ),
        in_specs=[any_space] * 7,
        out_specs=(vmem, vmem),
        scratch_shapes=[
            pltpu.VMEM((4, HALOS, HALF), BF16),
            pltpu.VMEM((4, HALOS), jnp.int32),
            pltpu.VMEM((4, HALOS), jnp.int32),
            pltpu.VMEM((4, K, HALOS), jnp.int32),
            pltpu.VMEM((4, HALOS), jnp.int32),
            pltpu.VMEM((4, HALOS), jnp.int32),
            pltpu.VMEM((2, 2, CANDS, HALF), BF16),
            pltpu.VMEM((4 * HALF, CANDS), BF16),
            pltpu.VMEM((2 * PEERS, SLOTS, HALF), BF16),
            pltpu.VMEM((2 * PEERS, SLOTS, HALF), BF16),
            pltpu.VMEM((PEERS, 1, HALF), F32),
            pltpu.VMEM((PEERS, 1, HALF), F32),
            pltpu.VMEM((2 * PEERS, SLOTS, HALF), BF16),
            pltpu.VMEM((2 * PEERS, SLOTS, HALF), BF16),
            pltpu.VMEM((PEERS, 1, HALF), F32),
            pltpu.VMEM((2 * PEERS, 1, HALF), F32),
            pltpu.VMEM((2, 2 * HALOS, HALF), F32),
            pltpu.VMEM((2, 2 * HALOS, REQS), BF16),
            pltpu.VMEM((PLANE, CANDS), F32),
            pltpu.VMEM((REQS, CANDS), BF16),
            pltpu.VMEM((REQS, HALF), F32),
            pltpu.VMEM((REQS, HALF), F32),
            pltpu.VMEM((REQS, 2 * HALF), F32),
            pltpu.VMEM((REQS, CANDS), F32),
            pltpu.VMEM((2, 2 * HALOS, HALF), F32),
            dma((6,)), dma, dma, dma, dma, dma((8,)), dma, dma((8,)), dma, dma, dma, dma,
            pltpu.SemaphoreType.REGULAR,
            dma, dma((8,)),
        ],
        compiler_params=pltpu.CompilerParams(collective_id=0, has_side_effects=True),
    )(halo_rows, unmatched, owner_id[:, :, 0], jnp.swapaxes(cand_index, 1, 2), lengths, choice_index, desc_rows)
    return pl.pallas_call(
        write_out,
        name="write",
        out_shape=(
            jax.ShapeDtypeStruct(halo_rows.shape, BF16),
            jax.ShapeDtypeStruct(unmatched.shape, BF16),
        ),
        in_specs=[vmem, vmem],
        out_specs=(any_space, any_space),
        scratch_shapes=[dma((2,))],
    )(pltpu.with_memory_space_constraint(out, pltpu.VMEM), pltpu.with_memory_space_constraint(best, pltpu.VMEM))


def solution(mesh):
    in_specs = (
        P(None, "space", "rep"),
        P(None, "space"),
        P(None, "space", None),
        P(None, "space", None),
        P(None, "space"),
        P(None, "space"),
        P(None, "space", "rep"),
    )
    out_specs = (P(None, "space", "rep"), P(None, "space"))
    return jax.shard_map(body, mesh=mesh, in_specs=in_specs, out_specs=out_specs, check_vma=False)
```
